512 devices in a mesh: grp: 4 (over y_hi, core), gx: 32 (over y_lo, z), gy: 4 (over x).
Axes of the slice: x: 4, y: 4 (y_hi: 2, y_lo: 2; y = y_hi * 2 + y_lo), z: 16, core: 2. Of those that a mesh axis runs over, the one named last changes fastest.
Arguments:
- sources: float32 [4, 128, 32, 512], P('grp', 'gx', 'gy'), may hold values from -4.5 to 5.5
- diagonal: float32 [128, 32, 512], P('gx', 'gy'), may hold values from 0.02 to 0.3
- coarse_ids: int32 [128, 32, 512], P('gx', 'gy'), may hold values from 0 to 255, as said below
- coarse_inverse: float32 [256, 256], replicated, may hold values from -1 to 3
- omega_rows: float32 [4, 32], replicated, may hold values from -5 to 5
- psi: float32 [32, 128, 32, 512], P(None, 'gx', 'gy', 'grp'), may hold values from -0.00390625 to 0.00390625
- phi: float32 [64, 128, 32, 512], P(None, 'gx', 'gy', 'grp'), may hold values from -0.00390625 to 0.00390625
- xi_cols: float32 [64, 4], replicated, may hold values from -5 to 5
- range_sketch: float32 [32, 128, 32, 512], P(None, 'gx', 'gy', 'grp'), may hold values from -3 to 3
- core_sketch: float32 [64, 64], replicated, may hold values from -2 to 2
Outputs:
- range_new: float32 [32, 128, 32, 512], P(None, 'gx', 'gy', 'grp')
- corange_cols: float32 [32, 4], replicated
- core_new: float32 [64, 64], replicated
The draws below stay inside these ranges and needn't reach their ends.
Inputs may be any that keep to these rules, and one draw needn't show every extreme that they name: `coarse_ids`: the grid is cut into 4, 4 and 16 non-empty ranges of consecutive cells along the three dimensions; coarse cell (a * 4 + b) * 16 + c is the box of ranges a, b, c.
All inputs are finite; a program needn't handle non-finite values.
Results may differ from the reference program's by a relative error of at most 0.0003.
Values sent between devices are 32-bit elements; how exact they have to be, the bound alone decides.
A program may use at most 64 MiB of HBM per device.

```python
import math
import jax
import jax.numpy as jnp
from jax import lax

NZ = 512
OUTER = 2
SWEEPS = 4
XY_CUTS = 4
Z_CUTS = 16
RANGE = 32
CORANGE = 32
CORE = 64
SNAPS = 4
NX = 128
NY = 32
COARSE = 256


def cut_ranks(key, length, pieces):
    chosen = jax.random.permutation(key, length - 1)[:pieces - 1] + 1
    bounds = jnp.sort(chosen)
    places = jnp.arange(length, dtype=jnp.int32)
    return jnp.sum((places[:, None] >= bounds[None, :]).astype(jnp.int32), axis=1)


def draw_coarse_ids(key, part):
    key_first = jax.random.fold_in(key, 11)
    key_second = jax.random.fold_in(key, 12)
    key_third = jax.random.fold_in(key, 13)
    ranks_x = cut_ranks(key_first, NX, XY_CUTS)
    ranks_y = cut_ranks(key_second, NY, XY_CUTS)
    ranks_z = cut_ranks(key_third, NZ, Z_CUTS)
    combined = (ranks_x[:, None, None] * XY_CUTS + ranks_y[None, :, None]) * Z_CUTS + ranks_z[None, None, :]
    return combined.astype(jnp.int32)


def draw_coarse_inverse(key, part):
    key_diag = jax.random.fold_in(key, 21)
    key_off = jax.random.fold_in(key, 22)
    diag_part = jnp.exp(jax.random.uniform(key_diag, (COARSE,), jnp.float32, math.log(0.5), math.log(2.0)))
    off_part = jax.random.truncated_normal(key_off, -4.0, 4.0, (COARSE, COARSE), jnp.float32) * (0.5 / math.sqrt(COARSE))
    return off_part + jnp.diag(diag_part)


def draw_sources(key, part):
    extent = (SNAPS, NX, NY, NZ)
    return jax.random.truncated_normal(key, -5.0, 5.0, extent, jnp.float32) + 0.5


def steps_of(own_key, shape, cuts, smallest, largest):
    factor_of, own = 1.0, jax.random.fold_in(own_key, 6)
    for axis_at, blocks in cuts:
        heights = jnp.exp(jax.random.uniform(jax.random.fold_in(own, axis_at), (blocks,), jnp.float32, smallest / len(cuts), largest / len(cuts)))
        factor_of = factor_of * jnp.repeat(heights, shape[axis_at] // blocks).reshape([-1 if axis == axis_at else 1 for axis in range(len(shape))])
    return factor_of


def gaussian(key, shape, width, most, shards=(), kind=jnp.bfloat16):
    loudness = steps_of(key, shape, shards, -0.22, 0.18) if shards else 1.0
    entries = jax.random.normal(key, shape, jnp.float32) * width * loudness
    return jnp.minimum(jnp.maximum(entries, -most), most).astype(kind)


def setup_inputs(seed: int = 0) -> dict:
    seeds = jax.random.split(jax.random.key(seed), 11)
    sources = draw_sources(jax.random.fold_in(seeds[10], 71), 0)
    diagonal = jnp.clip(jnp.exp(math.log(0.3) - 2.7080503 * jax.random.uniform(seeds[1], (NX, NY, NZ), jnp.float32) ** steps_of(seeds[1], (NX, NY, NZ), ((0, 32), (1, 4)), -0.2, 0.2)), 0.02, 0.3)
    coarse_ids = draw_coarse_ids(jax.random.fold_in(seeds[10], 71), 0)
    coarse_inverse = draw_coarse_inverse(jax.random.fold_in(seeds[10], 71), 0)
    omega_rows = gaussian(seeds[4], (SNAPS, RANGE), 1.0, 5.0, (), jnp.float32)
    psi = gaussian(seeds[5], (CORANGE, NX, NY, NZ), (NX * NY * NZ) ** -0.5, 0.00390625, ((1, 32), (2, 4), (3, 4)), jnp.float32)
    phi = gaussian(seeds[6], (CORE, NX, NY, NZ), (NX * NY * NZ) ** -0.5, 0.00390625, ((1, 32), (2, 4), (3, 4)), jnp.float32)
    xi_cols = gaussian(seeds[7], (CORE, SNAPS), 1.0, 5.0, (), jnp.float32)
    range_sketch = gaussian(seeds[8], (RANGE, NX, NY, NZ), 0.5, 3.0, ((1, 32), (2, 4), (3, 4)), jnp.float32)
    core_sketch = gaussian(seeds[9], (CORE, CORE), 0.3, 2.0, (), jnp.float32)
    return dict(sources=sources, diagonal=diagonal, coarse_ids=coarse_ids, coarse_inverse=coarse_inverse, omega_rows=omega_rows, psi=psi, phi=phi, xi_cols=xi_cols, range_sketch=range_sketch, core_sketch=core_sketch)


jacobi_weight = 2.0 / 3.0


def apply_operator(values, diagonal):
    padded = jnp.pad(values, 1)
    beside = padded[2:, 1:-1, 1:-1] + padded[:-2, 1:-1, 1:-1]
    beside = beside + padded[1:-1, 2:, 1:-1] + padded[1:-1, :-2, 1:-1]
    beside = beside + padded[1:-1, 1:-1, 2:] + padded[1:-1, 1:-1, :-2]
    return (6.0 + diagonal) * values - beside


def solve_snapshot(source, diagonal, coarse_ids, coarse_inverse):
    cell_count = NX * NY * NZ
    pressure = jnp.zeros_like(source)
    flat_ids = coarse_ids.reshape(-1).astype(jnp.int32)
    for outer_step in range(OUTER):
        residual = source - apply_operator(pressure, diagonal)
        coarse_rhs = jax.ops.segment_sum(residual.reshape(-1), flat_ids, num_segments=COARSE)
        correction = jnp.dot(coarse_inverse, coarse_rhs * (COARSE / cell_count), precision=lax.Precision.HIGHEST)
        pressure = pressure + correction[coarse_ids]
        for sweep_step in range(SWEEPS):
            pressure = pressure + jacobi_weight * (source - apply_operator(pressure, diagonal)) / (6.0 + diagonal)
    return pressure


def reference(sources, diagonal, coarse_ids, coarse_inverse, omega_rows, psi, phi, xi_cols, range_sketch, core_sketch):
    snapshots = jnp.stack([solve_snapshot(sources[index], diagonal, coarse_ids, coarse_inverse) for index in range(SNAPS)])
    range_new = range_sketch + jnp.einsum("tk,txyz->kxyz", omega_rows, snapshots, precision=lax.Precision.HIGHEST)
    corange_cols = jnp.einsum("lxyz,txyz->lt", psi, snapshots, precision=lax.Precision.HIGHEST)
    core_images = jnp.einsum("sxyz,txyz->st", phi, snapshots, precision=lax.Precision.HIGHEST)
    core_new = core_sketch + jnp.dot(core_images, xi_cols.T, precision=lax.Precision.HIGHEST)
    return range_new, corange_cols, core_new
```

```python
import functools

import jax
import jax.numpy as jnp
from jax import lax
from jax.experimental import pallas as pl
from jax.experimental.pallas import tpu as pltpu
from jax.sharding import PartitionSpec as P

OUTER = 2
SWEEPS = 4
XY_CUTS = 4
Z_CUTS = 16
HALO = 4
LANES = 128
THIRD = 1.0 / 3.0
TWO_THIRDS = 2.0 / 3.0

f32 = jnp.float32
bf16 = jnp.bfloat16
MESH = pl.DeviceIdType.MESH
HIGHEST = lax.Precision.HIGHEST
NT = (((1,), (1,)), ((), ()))
NN = (((1,), (0,)), ((), ()))


def dot(a, b, dims, precision=None):
    return lax.dot_general(a, b, dims, precision=precision, preferred_element_type=f32)


def split3(x):
    high = x.astype(bf16)
    rest = x - high.astype(f32)
    middle = rest.astype(bf16)
    low = (rest - middle.astype(f32)).astype(bf16)
    return high, middle, low


def iota(shape, dim):
    return lax.broadcasted_iota(jnp.int32, shape, dim)


def kernel(
    sizes,
    source_ref,
    diagonal_ref,
    ids_ref,
    inverse_ref,
    omega_ref,
    psi_hbm,
    phi_hbm,
    xi_ref,
    range_hbm,
    core_ref,
    range_out,
    corange_out,
    core_out,
    rows_k,
    range_in,
    range_done,
    ext_s,
    ext_d,
    ext_p,
    weight,
    weighted_q,
    field_a,
    field_b,
    final,
    snap,
    packed,
    reduced,
    ranks,
    ranks_in,
    map_zt,
    map_g,
    sum_send,
    zsum,
    psum,
    out_send,
    zout,
    pout,
    local_sem,
    halo_send,
    halo_recv,
    sum_send_sem,
    sum_recv_sem,
    snap_send,
    snap_recv,
):
    n_grp, n_gx, n_gy, n_z, total_cells = sizes
    n_low = n_gx // n_z
    rows_x, rows_y, cells_z = source_ref.shape
    per_k = rows_x * rows_y
    k_psi, k_phi = psi_hbm.shape[0] // per_k, phi_hbm.shape[0] // per_k
    k_all = k_psi + k_phi
    coarse = inverse_ref.shape[0]
    grp, gx, gy = lax.axis_index("grp"), lax.axis_index("gx"), lax.axis_index("gy")
    z_at = lax.rem(gx, n_z)
    low_at = lax.div(gx, n_z)

    z_peers = [
        (grp, low_at * n_z + lax.rem(z_at + i, n_z), gy) for i in range(1, n_z)
    ]
    plane = []
    for i in range(n_grp):
        for j in range(n_low):
            for k in range(n_gy):
                if i or j or k:
                    who = (
                        lax.rem(grp + i, n_grp),
                        lax.rem(gx + j * n_z, n_gx),
                        lax.rem(gy + k, n_gy),
                    )
                    plane.append(((i, j, k), who))
    own_plane = [who for (i, j, k), who in plane if i == 0]
    sides = []
    for ex in (-1, 0, 1):
        for ey in (-1, 0, 1):
            if ex or ey:
                who = (grp, lax.rem(gx + ex + n_gx, n_gx), lax.rem(gy + ey + n_gy, n_gy))
                sides.append(((ex, ey), who))
    everyone = z_peers + [who for _, who in plane] + [who for _, who in sides]
    barrier = pltpu.get_barrier_semaphore()
    for who in everyone:
        pl.semaphore_signal(barrier, inc=1, device_id=who, device_id_type=MESH)

    def remote(src, dst, send, recv, who):
        copy = pltpu.make_async_remote_copy(
            src_ref=src, dst_ref=dst, send_sem=send, recv_sem=recv,
            device_id=who, device_id_type=MESH,
        )
        copy.start()
        return copy

    def wait_bytes(ref, sem):
        pltpu.make_async_copy(ref, ref, sem).wait()

    loads = [
        pltpu.make_async_copy(psi_hbm, rows_k.at[pl.ds(0, k_psi * per_k)], local_sem.at[0]),
        pltpu.make_async_copy(phi_hbm, rows_k.at[pl.ds(k_psi * per_k, k_phi * per_k)], local_sem.at[1]),
        pltpu.make_async_copy(range_hbm, range_in, local_sem.at[2]),
    ]
    for load in loads:
        load.start()

    tile = (rows_y, LANES)
    sub = iota(tile, 0)
    lane = iota(tile, 1)
    box_lane = lane // Z_CUTS
    box = [jnp.broadcast_to(ids_ref[x, :, 0:1] // Z_CUTS, tile) for x in range(rows_x)]
    own_y = (box[0] % XY_CUTS).astype(f32)
    own_x = jnp.zeros(tile, f32)
    for x in range(rows_x):
        own_x = jnp.where(sub == x, (box[x] // XY_CUTS).astype(f32), own_x)
    ranks[0] = own_y
    ranks[1] = own_x
    rank_z = ids_ref[0, 0:1, :] % Z_CUTS
    map_zt[...] = jnp.where(
        iota((LANES, cells_z), 0) % Z_CUTS == rank_z, 1.0, 0.0
    ).astype(bf16)
    map_g[...] = jnp.where(
        iota((coarse, cells_z), 0) % Z_CUTS == rank_z, 1.0, 0.0
    ).astype(bf16)

    def along_z(values):
        parts = dot(jnp.concatenate(split3(values), axis=0), map_zt[...], NT)
        n = values.shape[0]
        return parts[:n] + parts[n : 2 * n] + parts[2 * n :]

    def to_boxes(terms):
        halves = []
        for first in (0, LANES // Z_CUTS):
            total = jnp.zeros(tile, f32)
            for rows, count in terms:
                total = total + rows * count(box_lane + first)
            halves.append(jnp.sum(total, axis=0, keepdims=True))
        return halves

    def same(rank):
        return lambda cell: jnp.where(rank == cell, 1.0, 0.0)

    def start_sum(which, halves):
        for i in range(2):
            sum_send[which, 0, pl.ds(i, 1), :] = halves[i]
        zsum[which, z_at] = sum_send[which, 0]
        for who in z_peers:
            remote(sum_send.at[which, 0], zsum.at[which, z_at],
                   sum_send_sem.at[which, 0], sum_recv_sem.at[which, 0], who)

    def middle_sum(which):
        wait_bytes(zsum.at[which, pl.ds(0, n_z - 1)], sum_recv_sem.at[which, 0])
        total = zsum[which, 0]
        for i in range(1, n_z):
            total = total + zsum[which, i]
        sum_send[which, 1] = total
        at = low_at * n_gy + gy
        psum[which, at] = sum_send[which, 1]
        for who in own_plane:
            remote(sum_send.at[which, 1], psum.at[which, at],
                   sum_send_sem.at[which, 1], sum_recv_sem.at[which, 1], who)

    def end_sum(which):
        n = n_low * n_gy
        wait_bytes(psum.at[which, pl.ds(0, n - 1)], sum_recv_sem.at[which, 1])
        total = psum[which, 0]
        for i in range(1, n):
            total = total + psum[which, i]
        return total * (coarse / total_cells)

    values = along_z(source_ref[...].reshape(per_k, cells_z))
    first_terms = [
        (values[x * rows_y : (x + 1) * rows_y], same(box[x])) for x in range(rows_x)
    ]
    halves = to_boxes(first_terms)

    pl.semaphore_wait(barrier, len(everyone))
    start_sum(0, halves)

    halo_copies = []
    y_from = {-1: pl.ds(0, HALO), 0: pl.ds(0, rows_y), 1: pl.ds(rows_y - HALO, HALO)}
    y_to = {-1: pl.ds(rows_y, HALO), 0: pl.ds(0, rows_y), 1: pl.ds(rows_y + HALO, HALO)}

    def x_rows(ex, depth):
        if ex == 0:
            return 0, HALO, rows_x
        if ex == 1:
            return rows_x - depth, HALO - depth, depth
        return 0, HALO + rows_x, depth

    def send_sides(src, ext, depth, base):
        for n, ((ex, ey), who) in enumerate(sides):
            first, to, count = x_rows(ex, depth - (1 if ex and ey else 0))
            halo_copies.append(
                remote(src.at[pl.ds(first, count), y_from[ey], :],
                       ext.at[pl.ds(to, count), y_to[ey], :],
                       halo_send.at[base + n], halo_recv.at[base + n], who)
            )

    n_rank = 0
    for (ex, ey), who in sides:
        if not (ex and ey):
            halo_copies.append(
                remote(ranks, ranks_in.at[n_rank],
                       halo_send.at[24 + n_rank], halo_recv.at[24 + n_rank], who)
            )
            n_rank += 1
    send_sides(diagonal_ref, ext_d, HALO - 1, 0)
    send_sides(source_ref, ext_s, HALO - 1, 8)
    ext_d[pl.ds(HALO, rows_x), pl.ds(0, rows_y), :] = diagonal_ref[...]
    ext_s[pl.ds(HALO, rows_x), pl.ds(0, rows_y), :] = source_ref[...]

    middle_sum(0)

    for copy in halo_copies:
        copy.wait_recv()
    far = -100.0
    x_after = jnp.where(gx == n_gx - 1, far, ranks_in[0, 1])
    y_after = jnp.where(gy == n_gy - 1, far, ranks_in[1, 0])
    y_before = jnp.where(gy == 0, far, ranks_in[2, 0])
    x_before = jnp.where(gx == 0, far, ranks_in[3, 1])
    rank_x = []
    for rows in (x_before, own_x, x_after):
        for x in range(rows_x):
            rank_x.append(jnp.broadcast_to(rows[x : x + 1], tile))
    halo_y = jnp.where(sub < HALO, y_after, y_before)
    rank_y = jnp.concatenate([own_y, halo_y], axis=0)
    wide = (2 * rows_y, cells_z)
    n_ext = rows_x + 2 * HALO

    def widen(column):
        return jnp.concatenate([column] * (cells_z // LANES), axis=-1)

    def widen_x(rows):
        rows = widen(rows)
        return jnp.concatenate([rows, rows], axis=0)

    rank_y_wide = widen(rank_y)
    rank_x_wide = [widen_x(rows) for rows in rank_x]
    for r in range(1, n_ext - 1):
        here = (rank_x_wide[r] >= 0.0) & (rank_y_wide >= 0.0)
        w = jnp.where(here, TWO_THIRDS / (6.0 + ext_d[r]), 0.0)
        weight[r] = w
        weighted_q[r] = jnp.where(here, w * ext_s[r], 0.0)

    y_up = pltpu.roll(rank_y, 2 * rows_y - 1, 0)[:rows_y]
    y_down = pltpu.roll(rank_y, 1, 0)[:rows_y]

    def beside(x):
        r = HALO + x
        ranks_of = [
            rank_x[r - 1] * XY_CUTS + own_y,
            rank_x[r + 1] * XY_CUTS + own_y,
            rank_x[r] * XY_CUTS + y_up,
            rank_x[r] * XY_CUTS + y_down,
        ]

        def count(cell):
            cell = cell.astype(f32)
            return sum(jnp.where(rank == cell, 1.0, 0.0) for rank in ranks_of)

        return count

    z_lane = iota(wide, 1)

    def z_pair(values, z_lane):
        before = jnp.where(z_lane == 0, 0.0, pltpu.roll(values, 1, 1))
        after = jnp.where(z_lane == cells_z - 1, 0.0, pltpu.roll(values, cells_z - 1, 1))
        return before + after

    def correct(which, store):
        rhs = end_sum(which)
        top = jnp.broadcast_to(rhs[0:1], (8, LANES))
        bottom = jnp.broadcast_to(rhs[1:2], (8, LANES))
        solved = dot(top, inverse_ref[:, 0:LANES], NT, HIGHEST)
        solved = solved + dot(bottom, inverse_ref[:, LANES:], NT, HIGHEST)
        pairs = XY_CUTS * XY_CUTS
        row = iota((pairs, coarse), 0)
        column = iota((pairs, coarse), 1)
        spread = jnp.where(
            column // Z_CUTS == row, jnp.broadcast_to(solved[0:1], (pairs, coarse)), 0.0
        )
        parts = dot(jnp.concatenate(split3(spread), axis=0), map_g[...], NN)
        boxes = parts[:pairs] + parts[pairs : 2 * pairs] + parts[2 * pairs :]
        by_x = []
        for a in range(XY_CUTS):
            picked = jnp.zeros(wide, f32)
            for b in range(XY_CUTS):
                line = boxes[a * XY_CUTS + b : a * XY_CUTS + b + 1]
                picked = jnp.where(rank_y_wide == float(b), jnp.broadcast_to(line, wide), picked)
            by_x.append(picked)
        for r in range(n_ext):
            picked = jnp.zeros(wide, f32)
            for a in range(XY_CUTS):
                picked = jnp.where(rank_x_wide[r] == float(a), by_x[a], picked)
            store(r, picked)

    def sweep(old, new, r):
        here = old[r]
        around = old[r - 1] + old[r + 1]
        around = around + pltpu.roll(here, 1, 0) + pltpu.roll(here, 2 * rows_y - 1, 0)
        around = around + z_pair(here, z_lane)
        new[r] = here * THIRD + weighted_q[r] + weight[r] * around

    def smooth(last):
        fields = (field_a, field_b)
        for s in range(SWEEPS):
            for r in range(1 + s, n_ext - 1 - s):
                if s == SWEEPS - 1:
                    last(r, fields[s % 2])
                else:
                    sweep(fields[s % 2], fields[1 - s % 2], r)

    own_lane = iota((rows_y, cells_z), 1)

    def last_value(r, old):
        here = old[r]
        around = old[r - 1, pl.ds(0, rows_y), :] + old[r + 1, pl.ds(0, rows_y), :]
        beside_y = pltpu.roll(here, 1, 0) + pltpu.roll(here, 2 * rows_y - 1, 0)
        here = here[:rows_y]
        around = around + beside_y[:rows_y] + z_pair(here, own_lane)
        own = pl.ds(0, rows_y)
        return here * THIRD + weighted_q[r, own, :] + weight[r, own, :] * around

    def store_first(r, picked):
        field_a[r] = picked

    correct(0, store_first)

    def last_first(r, old):
        ext_p[r, pl.ds(0, rows_y), :] = last_value(r, old)

    smooth(last_first)

    terms, stack = [], []
    for x in range(rows_x):
        p = ext_p[HALO + x, pl.ds(0, rows_y), :]
        stack.append(source_ref[x] - (6.0 + diagonal_ref[x]) * p + z_pair(p, own_lane))
    for x in range(rows_x):
        stack.append(ext_p[HALO + x, pl.ds(0, rows_y), :])
    values = along_z(jnp.concatenate(stack, axis=0))
    for x in range(2 * rows_x):
        count = same(box[x]) if x < rows_x else beside(x - rows_x)
        terms.append((values[x * rows_y : (x + 1) * rows_y], count))
    start_sum(1, to_boxes(terms))
    pressure_copies = len(halo_copies)
    send_sides(ext_p.at[pl.ds(HALO, rows_x), pl.ds(0, rows_y), :], ext_p, HALO, 16)

    for load in loads[:2]:
        load.wait()

    def pack(at, carry):
        for kt in range(k_all // 8):
            packed[kt, at] = rows_k[pl.ds(kt * 8 * per_k + at, 8, stride=per_k), :]
        return carry

    lax.fori_loop(0, per_k, pack, 0)
    middle_sum(1)
    for copy in halo_copies[pressure_copies:]:
        copy.wait_recv()

    def store_second(r, picked):
        here = (rank_x_wide[r] >= 0.0) & (rank_y_wide >= 0.0)
        field_a[r] = picked + jnp.where(here, ext_p[r], 0.0)

    correct(1, store_second)

    def last_second(r, old):
        final[pl.ds((r - HALO) * rows_y, rows_y), :] = last_value(r, old)

    smooth(last_second)

    snap_copies = []
    own_cells = pl.ds(pl.multiple_of(grp * per_k, per_k), per_k)
    for i in range(1, n_grp):
        other = lax.rem(grp + i, n_grp)
        lanes = pl.ds(pl.multiple_of(other * LANES, LANES), LANES)
        snap_copies.append(
            remote(final.at[:, lanes], snap.at[own_cells],
                   snap_send.at[i - 1], snap_recv.at[0], (other, gx, gy))
        )
    own_lanes = pl.ds(pl.multiple_of(grp * LANES, LANES), LANES)
    snap[own_cells, :] = final[:, own_lanes]
    wait_bytes(snap.at[pl.ds(0, (n_grp - 1) * per_k)], snap_recv.at[0])

    group = 6
    for base in range(0, k_all // 8, group):

        def step(at, carry):
            rows = [
                jnp.broadcast_to(snap[pl.ds(t * per_k + at, 1), :], (8, LANES))
                for t in range(n_grp)
            ]
            out = []
            for n in range(group):
                taken = packed[base + n, at]
                for t in range(n_grp):
                    out.append(carry[n * n_grp + t] + taken * rows[t])
            return tuple(out)

        zeros = tuple(jnp.zeros((8, LANES), f32) for _ in range(group * n_grp))
        sums = lax.fori_loop(0, per_k, step, zeros)
        for n in range(group):
            for t in range(n_grp):
                reduced[pl.ds(t * k_all + (base + n) * 8, 8), :] = sums[n * n_grp + t]
    sums = dot(jnp.ones((8, LANES), f32), reduced[...], NT, HIGHEST)[0:1]
    n_out = n_grp * k_all
    for i in range(n_out // LANES):
        out_send[0, pl.ds(i, 1), :] = sums[:, i * LANES : (i + 1) * LANES]
    for i in range(n_out // LANES, 4):
        out_send[0, pl.ds(i, 1), :] = jnp.zeros((1, LANES), f32)
    zout[z_at] = out_send[0]
    for who in z_peers:
        remote(out_send.at[0], zout.at[z_at], sum_send_sem.at[2, 0], sum_recv_sem.at[2, 0], who)

    loads[2].wait()

    def add_range(k, carry):
        total = range_in[k]
        for t in range(n_grp):
            total = total + omega_ref[t, k] * snap[pl.ds(t * per_k, per_k), :]
        range_done[k] = total
        return carry

    lax.fori_loop(0, range_in.shape[0], add_range, 0)
    store = pltpu.make_async_copy(range_done, range_out, local_sem.at[3])
    store.start()

    wait_bytes(zout.at[pl.ds(0, n_z - 1)], sum_recv_sem.at[2, 0])
    total = zout[0]
    for i in range(1, n_z):
        total = total + zout[i]
    out_send[1] = total
    at = (grp * n_low + low_at) * n_gy + gy
    pout[at] = out_send[1]
    for _, who in plane:
        remote(out_send.at[1], pout.at[at], sum_send_sem.at[2, 1], sum_recv_sem.at[2, 1], who)

    n_core = core_ref.shape[0]
    which_t = iota((n_out, LANES), 0) // k_all
    right = jnp.where(which_t == iota((n_out, LANES), 1) - n_core, 1.0, 0.0)
    lane_t = iota((n_out, 8), 1)
    pick = jnp.where(iota((n_out, 8), 0) // k_all == lane_t, 1.0, 0.0)
    xi = jnp.concatenate([xi_ref[...], jnp.zeros((n_core, 8 - n_grp), f32)], axis=1)
    xi = jnp.concatenate([xi, jnp.zeros((LANES - n_core, 8), f32)], axis=0)
    right = right + dot(pick, xi, NT, HIGHEST)
    left_row = iota((k_all, n_out), 0)
    left_pick = iota((k_all, n_out), 1) % k_all == left_row

    n_plane = n_grp * n_low * n_gy
    wait_bytes(pout.at[pl.ds(0, n_plane - 1)], sum_recv_sem.at[2, 1])
    total = pout[0]
    for i in range(1, n_plane):
        total = total + pout[i]
    line = jnp.concatenate([total[i : i + 1] for i in range(n_out // LANES)], axis=1)
    left = jnp.where(left_pick, jnp.broadcast_to(line, (k_all, n_out)), 0.0)
    result = dot(left, right, NN, HIGHEST)
    corange_out[...] = result[:k_psi, n_core : n_core + n_grp]
    core_out[...] = core_ref[...] + result[k_psi:, :n_core]

    store.wait()
    for copy in halo_copies:
        copy.wait_send()
    for copy in snap_copies:
        copy.wait_send()
    for which in range(2):
        wait_bytes(zsum.at[which, pl.ds(0, n_z - 1)], sum_send_sem.at[which, 0])
        wait_bytes(psum.at[which, pl.ds(0, n_low * n_gy - 1)], sum_send_sem.at[which, 1])
    wait_bytes(zout.at[pl.ds(0, n_z - 1)], sum_send_sem.at[2, 0])
    wait_bytes(pout.at[pl.ds(0, n_plane - 1)], sum_send_sem.at[2, 1])


def solution(mesh):
    n_grp, n_gx, n_gy = (mesh.shape[name] for name in ("grp", "gx", "gy"))
    n_z = min(16, n_gx // 2)
    n_low = n_gx // n_z

    def body(
        sources,
        diagonal,
        coarse_ids,
        coarse_inverse,
        omega_rows,
        psi,
        phi,
        xi_cols,
        range_sketch,
        core_sketch,
    ):
        _, rows_x, rows_y, cells_z = sources.shape
        total_cells = rows_x * n_gx * rows_y * n_gy * cells_z
        k_psi, k_phi = psi.shape[0], phi.shape[0]
        k_all = k_psi + k_phi
        k_range = range_sketch.shape[0]
        n_ext = rows_x + 2 * HALO
        per_k = rows_x * rows_y
        coarse = coarse_inverse.shape[0]
        vmem = pl.BlockSpec(memory_space=pltpu.VMEM)
        smem = pl.BlockSpec(memory_space=pltpu.SMEM)
        hbm = pl.BlockSpec(memory_space=pl.ANY)
        ext = pltpu.VMEM((n_ext, 2 * rows_y, cells_z), f32)
        call = pl.pallas_call(
            functools.partial(kernel, (n_grp, n_gx, n_gy, n_z, total_cells)),
            out_shape=(
                jax.ShapeDtypeStruct((k_range, per_k, LANES), f32),
                jax.ShapeDtypeStruct((k_psi, n_grp), f32),
                jax.ShapeDtypeStruct(core_sketch.shape, f32),
            ),
            in_specs=[vmem, vmem, vmem, vmem, smem, hbm, hbm, vmem, hbm, vmem],
            out_specs=(hbm, vmem, vmem),
            scratch_shapes=[
                pltpu.VMEM((k_all * per_k, LANES), f32),
                pltpu.VMEM((k_range, per_k, LANES), f32),
                pltpu.VMEM((k_range, per_k, LANES), f32),
                ext,
                ext,
                ext,
                ext,
                ext,
                ext,
                ext,
                pltpu.VMEM((per_k, cells_z), f32),
                pltpu.VMEM((n_grp * per_k, LANES), f32),
                pltpu.VMEM((k_all // 8, per_k, 8, LANES), f32),
                pltpu.VMEM((n_grp * k_all, LANES), f32),
                pltpu.VMEM((2, rows_y, LANES), f32),
                pltpu.VMEM((4, 2, rows_y, LANES), f32),
                pltpu.VMEM((LANES, cells_z), bf16),
                pltpu.VMEM((coarse, cells_z), bf16),
                pltpu.VMEM((2, 2, 2, LANES), f32),
                pltpu.VMEM((2, n_z, 2, LANES), f32),
                pltpu.VMEM((2, n_low * n_gy, 2, LANES), f32),
                pltpu.VMEM((2, 4, LANES), f32),
                pltpu.VMEM((n_z, 4, LANES), f32),
                pltpu.VMEM((n_grp * n_low * n_gy, 4, LANES), f32),
                pltpu.SemaphoreType.DMA((4,)),
                pltpu.SemaphoreType.DMA((28,)),
                pltpu.SemaphoreType.DMA((28,)),
                pltpu.SemaphoreType.DMA((3, 2)),
                pltpu.SemaphoreType.DMA((3, 2)),
                pltpu.SemaphoreType.DMA((n_grp - 1,)),
                pltpu.SemaphoreType.DMA((1,)),
            ],
            compiler_params=pltpu.CompilerParams(
                collective_id=0, has_side_effects=True
            ),
            name="two_level_sketch",
        )
        range_new, corange_cols, core_new = call(
            sources[0],
            diagonal,
            coarse_ids,
            coarse_inverse,
            omega_rows,
            psi.reshape(k_psi * per_k, LANES),
            phi.reshape(k_phi * per_k, LANES),
            xi_cols,
            range_sketch.reshape(k_range, per_k, LANES),
            core_sketch,
        )
        return range_new.reshape(range_sketch.shape), corange_cols, core_new

    return jax.shard_map(
        body,
        mesh=mesh,
        in_specs=(
            P("grp", "gx", "gy", None),
            P("gx", "gy", None),
            P("gx", "gy", None),
            P(),
            P(),
            P(None, "gx", "gy", "grp"),
            P(None, "gx", "gy", "grp"),
            P(),
            P(None, "gx", "gy", "grp"),
            P(),
        ),
        out_specs=(P(None, "gx", "gy", "grp"), P(), P()),
        check_vma=False,
    )
```

```python
import functools

import jax
import jax.numpy as jnp
from jax import lax
from jax.experimental import pallas as pl
from jax.experimental.pallas import tpu as pltpu
from jax.sharding import PartitionSpec as P

OUTER = 2
SWEEPS = 4
XY_CUTS = 4
Z_CUTS = 16
HALO = 4
LANES = 128
THIRD = 1.0 / 3.0
TWO_THIRDS = 2.0 / 3.0

f32 = jnp.float32
bf16 = jnp.bfloat16
MESH = pl.DeviceIdType.MESH
HIGHEST = lax.Precision.HIGHEST
NT = (((1,), (1,)), ((), ()))
NN = (((1,), (0,)), ((), ()))


def dot(a, b, dims, precision=None):
    return lax.dot_general(a, b, dims, precision=precision, preferred_element_type=f32)


def split3(x):
    high = x.astype(bf16)
    rest = x - high.astype(f32)
    middle = rest.astype(bf16)
    low = (rest - middle.astype(f32)).astype(bf16)
    return high, middle, low


def iota(shape, dim):
    return lax.broadcasted_iota(jnp.int32, shape, dim)


def kernel(
    sizes,
    source_hbm,
    diagonal_hbm,
    ids_hbm,
    inverse_hbm,
    omega_hbm,
    psi_hbm,
    phi_hbm,
    xi_hbm,
    range_hbm,
    core_hbm,
    range_done,
    corange_out,
    core_out,
    source_ref,
    diagonal_ref,
    ids_ref,
    inverse_ref,
    omega_ref,
    xi_ref,
    core_ref,
    rows_k,
    range_in,
    ext_s,
    ext_d,
    ext_p,
    weight,
    weighted_q,
    field_a,
    field_b,
    final,
    snap,
    packed,
    reduced,
    ranks,
    ranks_in,
    map_zt,
    map_g,
    sum_send,
    zsum,
    psum,
    out_send,
    zout,
    pout,
    local_sem,
    halo_send,
    halo_recv,
    sum_send_sem,
    sum_recv_sem,
    snap_send,
    snap_recv,
    chain,
):
    n_grp, n_gx, n_gy, n_z, total_cells = sizes
    n_low = n_gx // n_z
    rows_x, rows_y, cells_z = source_ref.shape
    per_k = rows_x * rows_y
    k_psi, k_phi = psi_hbm.shape[0] // per_k, phi_hbm.shape[0] // per_k
    k_all = k_psi + k_phi
    coarse = inverse_ref.shape[0]
    grp, gx, gy = lax.axis_index("grp"), lax.axis_index("gx"), lax.axis_index("gy")
    z_at = lax.rem(gx, n_z)
    low_at = lax.div(gx, n_z)

    z_peers = [
        (grp, low_at * n_z + lax.rem(z_at + i, n_z), gy) for i in range(1, n_z)
    ]
    plane = []
    for i in range(n_grp):
        for j in range(n_low):
            for k in range(n_gy):
                if i or j or k:
                    who = (
                        lax.rem(grp + i, n_grp),
                        lax.rem(gx + j * n_z, n_gx),
                        lax.rem(gy + k, n_gy),
                    )
                    plane.append(((i, j, k), who))
    own_plane = [who for (i, j, k), who in plane if i == 0]
    sides = []
    for ex in (-1, 0, 1):
        for ey in (-1, 0, 1):
            if ex or ey:
                who = (grp, lax.rem(gx + ex + n_gx, n_gx), lax.rem(gy + ey + n_gy, n_gy))
                sides.append(((ex, ey), who))
    grp_peers = [who for (i, j, k), who in plane if j == 0 and k == 0]
    near_z = [z_peers[i - 1] for i in range(1, n_z) if min(i, n_z - i) <= 2]
    near = own_plane + grp_peers + near_z + [who for _, who in sides]
    barrier = pltpu.get_barrier_semaphore()
    for who in near:
        pl.semaphore_signal(barrier, inc=1, device_id=who, device_id_type=MESH)

    def remote(src, dst, send, recv, who):
        copy = pltpu.make_async_remote_copy(
            src_ref=src, dst_ref=dst, send_sem=send, recv_sem=recv,
            device_id=who, device_id_type=MESH,
        )
        copy.start()
        return copy

    def wait_bytes(ref, sem):
        pltpu.make_async_copy(ref, ref, sem).wait()

    pairs = (
        (ids_hbm, ids_ref),
        (source_hbm, source_ref),
        (diagonal_hbm, diagonal_ref),
        (inverse_hbm, inverse_ref),
        (xi_hbm, xi_ref),
        (omega_hbm, omega_ref),
        (psi_hbm, rows_k.at[pl.ds(0, k_psi * per_k)]),
        (phi_hbm, rows_k.at[pl.ds(k_psi * per_k, k_phi * per_k)]),
        (range_hbm, range_in),
        (core_hbm, core_ref),
    )
    loads = [
        pltpu.make_async_copy(src, dst, local_sem.at[n]) for n, (src, dst) in enumerate(pairs)
    ]
    for load in loads:
        load.start()

    def take_loads(count):
        for _ in range(count):
            loads.pop(0).wait()

    take_loads(1)

    tile = (rows_y, LANES)
    sub = iota(tile, 0)
    lane = iota(tile, 1)
    box_lane = lane // Z_CUTS
    box = [jnp.broadcast_to(ids_ref[x, :, 0:1] // Z_CUTS, tile) for x in range(rows_x)]
    own_y = (box[0] % XY_CUTS).astype(f32)
    own_x = jnp.zeros(tile, f32)
    for x in range(rows_x):
        own_x = jnp.where(sub == x, (box[x] // XY_CUTS).astype(f32), own_x)
    ranks[0] = own_y
    ranks[1] = own_x
    rank_z = ids_ref[0, 0:1, :] % Z_CUTS
    map_zt[...] = jnp.where(
        iota((LANES, cells_z), 0) % Z_CUTS == rank_z, 1.0, 0.0
    ).astype(bf16)
    map_g[...] = jnp.where(
        iota((coarse, cells_z), 0) % Z_CUTS == rank_z, 1.0, 0.0
    ).astype(bf16)

    def along_z(values):
        parts = dot(jnp.concatenate(split3(values), axis=0), map_zt[...], NT)
        n = values.shape[0]
        return parts[:n] + parts[n : 2 * n] + parts[2 * n :]

    def to_boxes(terms):
        halves = []
        for first in (0, LANES // Z_CUTS):
            total = jnp.zeros(tile, f32)
            for rows, count in terms:
                total = total + rows * count(box_lane + first)
            halves.append(jnp.sum(total, axis=0, keepdims=True))
        return halves

    def same(rank):
        return lambda cell: jnp.where(rank == cell, 1.0, 0.0)

    plane_at = low_at * n_gy + gy
    n_plane = n_low * n_gy

    def start_sum(which, halves):
        for i in range(2):
            sum_send[which, 0, pl.ds(i, 1), :] = halves[i]
        psum[which, plane_at] = sum_send[which, 0]
        for who in own_plane:
            remote(sum_send.at[which, 0], psum.at[which, plane_at],
                   sum_send_sem.at[which, 0], sum_recv_sem.at[which, 0], who)

    def middle_sum(which):
        wait_bytes(psum.at[which, pl.ds(0, n_plane - 1)], sum_recv_sem.at[which, 0])
        total = psum[which, 0]
        for i in range(1, n_plane):
            total = total + psum[which, i]
        sum_send[which, 1] = total
        zsum[which, z_at] = sum_send[which, 1]
        for who in z_peers:
            remote(sum_send.at[which, 1], zsum.at[which, z_at],
                   sum_send_sem.at[which, 1], sum_recv_sem.at[which, 1], who)

    def end_sum(which):
        wait_bytes(zsum.at[which, pl.ds(0, n_z - 1)], sum_recv_sem.at[which, 1])
        total = zsum[which, 0]
        for i in range(1, n_z):
            total = total + zsum[which, i]
        return total * (coarse / total_cells)

    take_loads(1)

    values = along_z(source_ref[...].reshape(per_k, cells_z))
    first_terms = [
        (values[x * rows_y : (x + 1) * rows_y], same(box[x])) for x in range(rows_x)
    ]
    halves = to_boxes(first_terms)

    pl.semaphore_wait(barrier, len(near))
    start_sum(0, halves)

    take_loads(4)
    halo_copies = []
    y_from = {-1: pl.ds(0, HALO), 0: pl.ds(0, rows_y), 1: pl.ds(rows_y - HALO, HALO)}
    y_to = {-1: pl.ds(rows_y, HALO), 0: pl.ds(0, rows_y), 1: pl.ds(rows_y + HALO, HALO)}

    def x_rows(ex, depth):
        if ex == 0:
            return 0, HALO, rows_x
        if ex == 1:
            return rows_x - depth, HALO - depth, depth
        return 0, HALO + rows_x, depth

    def send_sides(src, ext, depth, base):
        for n, ((ex, ey), who) in enumerate(sides):
            first, to, count = x_rows(ex, depth - (1 if ex and ey else 0))
            halo_copies.append(
                remote(src.at[pl.ds(first, count), y_from[ey], :],
                       ext.at[pl.ds(to, count), y_to[ey], :],
                       halo_send.at[base + n], halo_recv.at[base + n], who)
            )

    n_rank = 0
    for (ex, ey), who in sides:
        if not (ex and ey):
            halo_copies.append(
                remote(ranks, ranks_in.at[n_rank],
                       halo_send.at[24 + n_rank], halo_recv.at[24 + n_rank], who)
            )
            n_rank += 1
    send_sides(diagonal_ref, ext_d, HALO - 1, 0)
    send_sides(source_ref, ext_s, HALO - 1, 8)
    ext_d[pl.ds(HALO, rows_x), pl.ds(0, rows_y), :] = diagonal_ref[...]
    ext_s[pl.ds(HALO, rows_x), pl.ds(0, rows_y), :] = source_ref[...]

    reach, level = 2, 0
    while reach < n_z // 2:
        for i in (reach, n_z - reach):
            pl.semaphore_signal(
                chain.at[level], inc=1, device_id=z_peers[i - 1], device_id_type=MESH
            )
        pl.semaphore_wait(chain.at[level], 2)
        reach, level = 2 * reach, level + 1

    middle_sum(0)

    for copy in halo_copies:
        copy.wait_recv()
    far = -100.0
    x_after = jnp.where(gx == n_gx - 1, far, ranks_in[0, 1])
    y_after = jnp.where(gy == n_gy - 1, far, ranks_in[1, 0])
    y_before = jnp.where(gy == 0, far, ranks_in[2, 0])
    x_before = jnp.where(gx == 0, far, ranks_in[3, 1])
    rank_x = []
    for rows in (x_before, own_x, x_after):
        for x in range(rows_x):
            rank_x.append(jnp.broadcast_to(rows[x : x + 1], tile))
    halo_y = jnp.where(sub < HALO, y_after, y_before)
    rank_y = jnp.concatenate([own_y, halo_y], axis=0)
    wide = (2 * rows_y, cells_z)
    n_ext = rows_x + 2 * HALO

    def widen(column):
        return jnp.concatenate([column] * (cells_z // LANES), axis=-1)

    def widen_x(rows):
        rows = widen(rows)
        return jnp.concatenate([rows, rows], axis=0)

    rank_y_wide = widen(rank_y)
    rank_x_wide = [widen_x(rows) for rows in rank_x]
    for r in range(1, n_ext - 1):
        here = (rank_x_wide[r] >= 0.0) & (rank_y_wide >= 0.0)
        w = jnp.where(here, TWO_THIRDS / (6.0 + ext_d[r]), 0.0)
        weight[r] = w
        weighted_q[r] = jnp.where(here, w * ext_s[r], 0.0)

    y_up = pltpu.roll(rank_y, 2 * rows_y - 1, 0)[:rows_y]
    y_down = pltpu.roll(rank_y, 1, 0)[:rows_y]

    def beside(x):
        r = HALO + x
        ranks_of = [
            rank_x[r - 1] * XY_CUTS + own_y,
            rank_x[r + 1] * XY_CUTS + own_y,
            rank_x[r] * XY_CUTS + y_up,
            rank_x[r] * XY_CUTS + y_down,
        ]

        def count(cell):
            cell = cell.astype(f32)
            return sum(jnp.where(rank == cell, 1.0, 0.0) for rank in ranks_of)

        return count

    z_lane = iota(wide, 1)

    def z_pair(values, z_lane):
        before = jnp.where(z_lane == 0, 0.0, pltpu.roll(values, 1, 1))
        after = jnp.where(z_lane == cells_z - 1, 0.0, pltpu.roll(values, cells_z - 1, 1))
        return before + after

    def correct(which, store):
        rhs = end_sum(which)
        top = jnp.broadcast_to(rhs[0:1], (8, LANES))
        bottom = jnp.broadcast_to(rhs[1:2], (8, LANES))
        solved = dot(top, inverse_ref[:, 0:LANES], NT, HIGHEST)
        solved = solved + dot(bottom, inverse_ref[:, LANES:], NT, HIGHEST)
        pairs = XY_CUTS * XY_CUTS
        row = iota((pairs, coarse), 0)
        column = iota((pairs, coarse), 1)
        spread = jnp.where(
            column // Z_CUTS == row, jnp.broadcast_to(solved[0:1], (pairs, coarse)), 0.0
        )
        parts = dot(jnp.concatenate(split3(spread), axis=0), map_g[...], NN)
        boxes = parts[:pairs] + parts[pairs : 2 * pairs] + parts[2 * pairs :]
        by_x = []
        for a in range(XY_CUTS):
            picked = jnp.zeros(wide, f32)
            for b in range(XY_CUTS):
                line = boxes[a * XY_CUTS + b : a * XY_CUTS + b + 1]
                picked = jnp.where(rank_y_wide == float(b), jnp.broadcast_to(line, wide), picked)
            by_x.append(picked)
        for r in range(n_ext):
            picked = jnp.zeros(wide, f32)
            for a in range(XY_CUTS):
                picked = jnp.where(rank_x_wide[r] == float(a), by_x[a], picked)
            store(r, picked)

    def sweep(old, new, r):
        here = old[r]
        around = old[r - 1] + old[r + 1]
        around = around + pltpu.roll(here, 1, 0) + pltpu.roll(here, 2 * rows_y - 1, 0)
        around = around + z_pair(here, z_lane)
        new[r] = here * THIRD + weighted_q[r] + weight[r] * around

    def smooth(last):
        fields = (field_a, field_b)
        for s in range(SWEEPS):
            for r in range(1 + s, n_ext - 1 - s):
                if s == SWEEPS - 1:
                    last(r, fields[s % 2])
                else:
                    sweep(fields[s % 2], fields[1 - s % 2], r)

    own_lane = iota((rows_y, cells_z), 1)

    def last_value(r, old):
        here = old[r]
        around = old[r - 1, pl.ds(0, rows_y), :] + old[r + 1, pl.ds(0, rows_y), :]
        beside_y = pltpu.roll(here, 1, 0) + pltpu.roll(here, 2 * rows_y - 1, 0)
        here = here[:rows_y]
        around = around + beside_y[:rows_y] + z_pair(here, own_lane)
        own = pl.ds(0, rows_y)
        return here * THIRD + weighted_q[r, own, :] + weight[r, own, :] * around

    def store_first(r, picked):
        field_a[r] = picked

    correct(0, store_first)

    def last_first(r, old):
        ext_p[r, pl.ds(0, rows_y), :] = last_value(r, old)

    smooth(last_first)

    terms, stack = [], []
    for x in range(rows_x):
        p = ext_p[HALO + x, pl.ds(0, rows_y), :]
        stack.append(source_ref[x] - (6.0 + diagonal_ref[x]) * p + z_pair(p, own_lane))
    for x in range(rows_x):
        stack.append(ext_p[HALO + x, pl.ds(0, rows_y), :])
    values = along_z(jnp.concatenate(stack, axis=0))
    for x in range(2 * rows_x):
        count = same(box[x]) if x < rows_x else beside(x - rows_x)
        terms.append((values[x * rows_y : (x + 1) * rows_y], count))
    start_sum(1, to_boxes(terms))
    pressure_copies = len(halo_copies)
    send_sides(ext_p.at[pl.ds(HALO, rows_x), pl.ds(0, rows_y), :], ext_p, HALO, 16)

    take_loads(2)

    def pack(at, carry):
        for kt in range(k_all // 8):
            packed[kt, at] = rows_k[pl.ds(kt * 8 * per_k + at, 8, stride=per_k), :]
        return carry

    lax.fori_loop(0, per_k, pack, 0)
    middle_sum(1)
    for copy in halo_copies[pressure_copies:]:
        copy.wait_recv()

    def store_second(r, picked):
        here = (rank_x_wide[r] >= 0.0) & (rank_y_wide >= 0.0)
        field_a[r] = picked + jnp.where(here, ext_p[r], 0.0)

    correct(1, store_second)

    def last_second(r, old):
        final[pl.ds((r - HALO) * rows_y, rows_y), :] = last_value(r, old)

    smooth(last_second)

    snap_copies = []
    own_cells = pl.ds(pl.multiple_of(grp * per_k, per_k), per_k)
    for i in range(1, n_grp):
        other = lax.rem(grp + i, n_grp)
        lanes = pl.ds(pl.multiple_of(other * LANES, LANES), LANES)
        snap_copies.append(
            remote(final.at[:, lanes], snap.at[own_cells],
                   snap_send.at[i - 1], snap_recv.at[0], (other, gx, gy))
        )
    own_lanes = pl.ds(pl.multiple_of(grp * LANES, LANES), LANES)
    snap[own_cells, :] = final[:, own_lanes]
    wait_bytes(snap.at[pl.ds(0, (n_grp - 1) * per_k)], snap_recv.at[0])

    group = 6
    for base in range(0, k_all // 8, group):

        def step(at, carry):
            rows = [
                jnp.broadcast_to(snap[pl.ds(t * per_k + at, 1), :], (8, LANES))
                for t in range(n_grp)
            ]
            out = []
            for n in range(group):
                taken = packed[base + n, at]
                for t in range(n_grp):
                    out.append(carry[n * n_grp + t] + taken * rows[t])
            return tuple(out)

        zeros = tuple(jnp.zeros((8, LANES), f32) for _ in range(group * n_grp))
        sums = lax.fori_loop(0, per_k, step, zeros)
        for n in range(group):
            for t in range(n_grp):
                reduced[pl.ds(t * k_all + (base + n) * 8, 8), :] = sums[n * n_grp + t]
    sums = dot(jnp.ones((8, LANES), f32), reduced[...], NT, HIGHEST)[0:1]
    n_out = n_grp * k_all
    for i in range(n_out // LANES):
        out_send[0, pl.ds(i, 1), :] = sums[:, i * LANES : (i + 1) * LANES]
    for i in range(n_out // LANES, 4):
        out_send[0, pl.ds(i, 1), :] = jnp.zeros((1, LANES), f32)
    all_at = grp * n_plane + plane_at
    pout[all_at] = out_send[0]
    for _, who in plane:
        remote(out_send.at[0], pout.at[all_at], sum_send_sem.at[2, 0], sum_recv_sem.at[2, 0], who)

    take_loads(2)

    def add_range(k, carry):
        total = range_in[k]
        for t in range(n_grp):
            total = total + omega_ref[t, k] * snap[pl.ds(t * per_k, per_k), :]
        range_done[k] = total
        return carry

    lax.fori_loop(0, range_in.shape[0], add_range, 0)

    n_all = n_grp * n_plane
    wait_bytes(pout.at[pl.ds(0, n_all - 1)], sum_recv_sem.at[2, 0])
    total = pout[0]
    for i in range(1, n_all):
        total = total + pout[i]
    out_send[1] = total
    zout[z_at] = out_send[1]
    for who in z_peers:
        remote(out_send.at[1], zout.at[z_at], sum_send_sem.at[2, 1], sum_recv_sem.at[2, 1], who)

    n_core = xi_ref.shape[1]
    by_t = iota((n_out, n_core), 0) // k_all
    right = jnp.zeros((n_out, n_core), f32)
    for t in range(n_grp):
        line = jnp.broadcast_to(xi_ref[pl.ds(t, 1), :], (n_out, n_core))
        right = jnp.where(by_t == t, line, right)
    core_pick = iota((k_phi, n_out), 1) % k_all == iota((k_phi, n_out), 0) + k_psi
    t_pick = iota((8, n_out), 1) // k_all == iota((8, n_out), 0)
    row_pick = iota((n_out, k_psi), 0) % k_all == iota((n_out, k_psi), 1)
    row_pick = jnp.where(row_pick, 1.0, 0.0)

    wait_bytes(zout.at[pl.ds(0, n_z - 1)], sum_recv_sem.at[2, 1])
    total = zout[0]
    for i in range(1, n_z):
        total = total + zout[i]
    line = jnp.concatenate([total[i : i + 1] for i in range(n_out // LANES)], axis=1)
    left = jnp.where(core_pick, jnp.broadcast_to(line, (k_phi, n_out)), 0.0)
    core_out[...] = core_ref[...] + dot(left, right, NN, HIGHEST)
    left = jnp.where(t_pick, jnp.broadcast_to(line, (8, n_out)), 0.0)
    corange_out[...] = dot(left, row_pick, NN, HIGHEST)[:n_grp]

    for copy in halo_copies:
        copy.wait_send()
    for copy in snap_copies:
        copy.wait_send()
    for which in range(2):
        wait_bytes(psum.at[which, pl.ds(0, n_plane - 1)], sum_send_sem.at[which, 0])
        wait_bytes(zsum.at[which, pl.ds(0, n_z - 1)], sum_send_sem.at[which, 1])
    wait_bytes(pout.at[pl.ds(0, n_all - 1)], sum_send_sem.at[2, 0])
    wait_bytes(zout.at[pl.ds(0, n_z - 1)], sum_send_sem.at[2, 1])


def finish(range_in, corange_in, core_in, range_out, corange_out, core_out, sems):
    pairs = ((range_in, range_out), (corange_in, corange_out), (core_in, core_out))
    stores = [pltpu.make_async_copy(src, dst, sems.at[n]) for n, (src, dst) in enumerate(pairs)]
    for store in stores:
        store.start()
    for store in stores:
        store.wait()


def solution(mesh):
    n_grp, n_gx, n_gy = (mesh.shape[name] for name in ("grp", "gx", "gy"))
    n_z = min(16, n_gx // 2)
    n_low = n_gx // n_z

    def body(
        sources,
        diagonal,
        coarse_ids,
        coarse_inverse,
        omega_rows,
        psi,
        phi,
        xi_cols,
        range_sketch,
        core_sketch,
    ):
        _, rows_x, rows_y, cells_z = sources.shape
        total_cells = rows_x * n_gx * rows_y * n_gy * cells_z
        k_psi, k_phi = psi.shape[0], phi.shape[0]
        k_all = k_psi + k_phi
        k_range = range_sketch.shape[0]
        n_ext = rows_x + 2 * HALO
        per_k = rows_x * rows_y
        coarse = coarse_inverse.shape[0]
        vmem = pl.BlockSpec(memory_space=pltpu.VMEM)
        hbm = pl.BlockSpec(memory_space=pl.ANY)
        ext = pltpu.VMEM((n_ext, 2 * rows_y, cells_z), f32)
        call = pl.pallas_call(
            functools.partial(kernel, (n_grp, n_gx, n_gy, n_z, total_cells)),
            out_shape=(
                pltpu.VMEM((k_range, per_k, LANES), f32),
                pltpu.VMEM((n_grp, k_psi), f32),
                pltpu.VMEM(core_sketch.shape, f32),
            ),
            in_specs=[hbm] * 10,
            out_specs=(vmem, vmem, vmem),
            scratch_shapes=[
                pltpu.VMEM((rows_x, rows_y, cells_z), f32),
                pltpu.VMEM((rows_x, rows_y, cells_z), f32),
                pltpu.VMEM((rows_x, rows_y, cells_z), jnp.int32),
                pltpu.VMEM(coarse_inverse.shape, f32),
                pltpu.SMEM(omega_rows.shape, f32),
                pltpu.VMEM((n_grp, xi_cols.shape[0]), f32),
                pltpu.VMEM(core_sketch.shape, f32),
                pltpu.VMEM((k_all * per_k, LANES), f32),
                pltpu.VMEM((k_range, per_k, LANES), f32),
                ext,
                ext,
                ext,
                ext,
                ext,
                ext,
                ext,
                pltpu.VMEM((per_k, cells_z), f32),
                pltpu.VMEM((n_grp * per_k, LANES), f32),
                pltpu.VMEM((k_all // 8, per_k, 8, LANES), f32),
                pltpu.VMEM((n_grp * k_all, LANES), f32),
                pltpu.VMEM((2, rows_y, LANES), f32),
                pltpu.VMEM((4, 2, rows_y, LANES), f32),
                pltpu.VMEM((LANES, cells_z), bf16),
                pltpu.VMEM((coarse, cells_z), bf16),
                pltpu.VMEM((2, 2, 2, LANES), f32),
                pltpu.VMEM((2, n_z, 2, LANES), f32),
                pltpu.VMEM((2, n_low * n_gy, 2, LANES), f32),
                pltpu.VMEM((2, 4, LANES), f32),
                pltpu.VMEM((n_z, 4, LANES), f32),
                pltpu.VMEM((n_grp * n_low * n_gy, 4, LANES), f32),
                pltpu.SemaphoreType.DMA((10,)),
                pltpu.SemaphoreType.DMA((28,)),
                pltpu.SemaphoreType.DMA((28,)),
                pltpu.SemaphoreType.DMA((3, 2)),
                pltpu.SemaphoreType.DMA((3, 2)),
                pltpu.SemaphoreType.DMA((n_grp - 1,)),
                pltpu.SemaphoreType.DMA((1,)),
                pltpu.SemaphoreType.REGULAR((2,)),
            ],
            compiler_params=pltpu.CompilerParams(
                collective_id=0, has_side_effects=True
            ),
            name="two_level_sketch",
        )
        range_new, corange_cols, core_new = call(
            sources[0],
            diagonal,
            coarse_ids,
            coarse_inverse,
            omega_rows,
            psi.reshape(k_psi * per_k, LANES),
            phi.reshape(k_phi * per_k, LANES),
            xi_cols.T,
            range_sketch.reshape(k_range, per_k, LANES),
            core_sketch,
        )
        range_new, corange_cols, core_new = pl.pallas_call(
            finish,
            out_shape=(
                jax.ShapeDtypeStruct((k_range, per_k, LANES), f32),
                jax.ShapeDtypeStruct((n_grp, k_psi), f32),
                jax.ShapeDtypeStruct(core_sketch.shape, f32),
            ),
            in_specs=[vmem] * 3,
            out_specs=(hbm, hbm, hbm),
            scratch_shapes=[pltpu.SemaphoreType.DMA((3,))],
            compiler_params=pltpu.CompilerParams(vmem_limit_bytes=1 << 21),
            name="finish",
        )(range_new, corange_cols, core_new)
        return range_new.reshape(range_sketch.shape), corange_cols.T, core_new

    return jax.shard_map(
        body,
        mesh=mesh,
        in_specs=(
            P("grp", "gx", "gy", None),
            P("gx", "gy", None),
            P("gx", "gy", None),
            P(),
            P(),
            P(None, "gx", "gy", "grp"),
            P(None, "gx", "gy", "grp"),
            P(),
            P(None, "gx", "gy", "grp"),
            P(),
        ),
        out_specs=(P(None, "gx", "gy", "grp"), P(), P()),
        check_vma=False,
    )
```

```python
import functools

import jax
import jax.numpy as jnp
from jax import lax
from jax.experimental import pallas as pl
from jax.experimental.pallas import tpu as pltpu
from jax.sharding import PartitionSpec as P

OUTER = 2
SWEEPS = 4
XY_CUTS = 4
Z_CUTS = 16
HALO = 4
LANES = 128
THIRD = 1.0 / 3.0
TWO_THIRDS = 2.0 / 3.0

f32 = jnp.float32
bf16 = jnp.bfloat16
MESH = pl.DeviceIdType.MESH
HIGHEST = lax.Precision.HIGHEST
NT = (((1,), (1,)), ((), ()))
NN = (((1,), (0,)), ((), ()))


def dot(a, b, dims, precision=None):
    return lax.dot_general(a, b, dims, precision=precision, preferred_element_type=f32)


def split3(x):
    high = x.astype(bf16)
    rest = x - high.astype(f32)
    middle = rest.astype(bf16)
    low = (rest - middle.astype(f32)).astype(bf16)
    return high, middle, low


def iota(shape, dim):
    return lax.broadcasted_iota(jnp.int32, shape, dim)


def kernel(
    sizes,
    source_hbm,
    diagonal_hbm,
    ids_hbm,
    inverse_hbm,
    omega_hbm,
    psi_hbm,
    phi_hbm,
    xi_hbm,
    range_hbm,
    core_hbm,
    range_done,
    corange_out,
    core_out,
    source_ref,
    diagonal_ref,
    ids_ref,
    inverse_ref,
    omega_ref,
    xi_ref,
    core_ref,
    rows_k,
    range_in,
    ext_s,
    ext_d,
    ext_p,
    weight,
    weighted_q,
    field_a,
    field_b,
    final,
    snap,
    packed,
    reduced,
    ranks,
    ranks_in,
    map_zt,
    map_g,
    sum_send,
    zsum,
    psum,
    out_send,
    zout,
    pout,
    local_sem,
    halo_send,
    halo_recv,
    sum_send_sem,
    sum_recv_sem,
    snap_send,
    snap_recv,
    chain,
    inverse_parts,
):
    n_grp, n_gx, n_gy, n_z, total_cells = sizes
    n_low = n_gx // n_z
    rows_x, rows_y, cells_z = source_ref.shape
    per_k = rows_x * rows_y
    k_psi, k_phi = psi_hbm.shape[0] // per_k, phi_hbm.shape[0] // per_k
    k_all = k_psi + k_phi
    coarse = inverse_ref.shape[0]
    grp, gx, gy = lax.axis_index("grp"), lax.axis_index("gx"), lax.axis_index("gy")
    z_at = lax.rem(gx, n_z)
    low_at = lax.div(gx, n_z)

    z_peers = [
        (grp, low_at * n_z + lax.rem(z_at + i, n_z), gy) for i in range(1, n_z)
    ]
    plane = []
    for i in range(n_grp):
        for j in range(n_low):
            for k in range(n_gy):
                if i or j or k:
                    who = (
                        lax.rem(grp + i, n_grp),
                        lax.rem(gx + j * n_z, n_gx),
                        lax.rem(gy + k, n_gy),
                    )
                    plane.append(((i, j, k), who))
    plane.sort(key=lambda peer: -(min(peer[0][0], n_grp - peer[0][0]) + peer[0][1]
                                  + min(peer[0][2], n_gy - peer[0][2])))
    own_plane = [who for (i, j, k), who in plane if i == 0]
    z_order = sorted(range(n_z - 1), key=lambda i: -min(i + 1, n_z - 1 - i))
    far_first = [z_peers[i] for i in z_order]
    sides = []
    for ex in (-1, 0, 1):
        for ey in (-1, 0, 1):
            if ex or ey:
                who = (grp, lax.rem(gx + ex + n_gx, n_gx), lax.rem(gy + ey + n_gy, n_gy))
                sides.append(((ex, ey), who))
    grp_peers = [who for (i, j, k), who in plane if j == 0 and k == 0]
    near_z = [z_peers[i - 1] for i in range(1, n_z) if min(i, n_z - i) <= 2]
    near = own_plane + grp_peers + near_z + [who for _, who in sides]
    pairs = (
        (ids_hbm, ids_ref),
        (source_hbm, source_ref),
        (diagonal_hbm, diagonal_ref),
        (inverse_hbm, inverse_ref),
        (xi_hbm, xi_ref),
        (omega_hbm, omega_ref),
        (psi_hbm, rows_k.at[pl.ds(0, k_psi * per_k)]),
        (phi_hbm, rows_k.at[pl.ds(k_psi * per_k, k_phi * per_k)]),
        (range_hbm, range_in),
        (core_hbm, core_ref),
    )
    loads = [
        pltpu.make_async_copy(src, dst, local_sem.at[n]) for n, (src, dst) in enumerate(pairs)
    ]
    for load in loads[:2]:
        load.start()
    barrier = pltpu.get_barrier_semaphore()
    for who in near:
        pl.semaphore_signal(barrier, inc=1, device_id=who, device_id_type=MESH)
    for load in loads[2:]:
        load.start()

    def remote(src, dst, send, recv, who):
        copy = pltpu.make_async_remote_copy(
            src_ref=src, dst_ref=dst, send_sem=send, recv_sem=recv,
            device_id=who, device_id_type=MESH,
        )
        copy.start()
        return copy

    ends = []

    def wait_bytes(ref, sem):
        pltpu.make_async_copy(ref, ref, sem).wait()

    def take_loads(count):
        for _ in range(count):
            loads.pop(0).wait()

    take_loads(1)

    tile = (rows_y, LANES)
    sub = iota(tile, 0)
    lane = iota(tile, 1)
    box_lane = lane // Z_CUTS
    box = [jnp.broadcast_to(ids_ref[x, :, 0:1] // Z_CUTS, tile) for x in range(rows_x)]
    own_y = (box[0] % XY_CUTS).astype(f32)
    own_x = jnp.zeros(tile, f32)
    for x in range(rows_x):
        own_x = jnp.where(sub == x, (box[x] // XY_CUTS).astype(f32), own_x)
    ranks[0] = own_y
    ranks[1] = own_x
    rank_z = ids_ref[0, 0:1, :] % Z_CUTS
    map_zt[...] = jnp.where(
        iota((LANES, cells_z), 0) % Z_CUTS == rank_z, 1.0, 0.0
    ).astype(bf16)
    map_g[...] = jnp.where(
        iota((coarse, cells_z), 0) % Z_CUTS == rank_z, 1.0, 0.0
    ).astype(bf16)

    def along_z(values):
        parts = dot(jnp.concatenate(split3(values), axis=0), map_zt[...], NT)
        n = values.shape[0]
        return parts[:n] + parts[n : 2 * n] + parts[2 * n :]

    def to_boxes(terms):
        halves = []
        for first in (0, LANES // Z_CUTS):
            total = jnp.zeros(tile, f32)
            for rows, count in terms:
                total = total + rows * count(box_lane + first)
            halves.append(jnp.sum(total, axis=0, keepdims=True))
        return halves

    def same(rank):
        return lambda cell: jnp.where(rank == cell, 1.0, 0.0)

    plane_at = low_at * n_gy + gy
    n_plane = n_low * n_gy

    def start_sum(which, halves):
        for i in range(2):
            sum_send[which, 0, pl.ds(i, 1), :] = halves[i]
        psum[which, plane_at] = sum_send[which, 0]
        for who in own_plane:
            remote(sum_send.at[which, 0], psum.at[which, plane_at],
                   sum_send_sem.at[which, 0], sum_recv_sem.at[which, 0], who)
        ends.append(lambda: wait_bytes(psum.at[which, pl.ds(0, n_plane - 1)], sum_send_sem.at[which, 0]))

    def middle_sum(which):
        wait_bytes(psum.at[which, pl.ds(0, n_plane - 1)], sum_recv_sem.at[which, 0])
        total = psum[which, 0]
        for i in range(1, n_plane):
            total = total + psum[which, i]
        sum_send[which, 1] = total
        zsum[which, z_at] = sum_send[which, 1]
        for who in far_first:
            remote(sum_send.at[which, 1], zsum.at[which, z_at],
                   sum_send_sem.at[which, 1], sum_recv_sem.at[which, 1], who)
        ends.append(lambda: wait_bytes(zsum.at[which, pl.ds(0, n_z - 1)], sum_send_sem.at[which, 1]))

    def end_sum(which):
        wait_bytes(zsum.at[which, pl.ds(0, n_z - 1)], sum_recv_sem.at[which, 1])
        total = zsum[which, 0]
        for i in range(1, n_z):
            total = total + zsum[which, i]
        return total * (coarse / total_cells)

    take_loads(1)

    values = along_z(source_ref[...].reshape(per_k, cells_z))
    first_terms = [
        (values[x * rows_y : (x + 1) * rows_y], same(box[x])) for x in range(rows_x)
    ]
    halves = to_boxes(first_terms)

    pl.semaphore_wait(barrier, len(near))
    reaches = []
    while 2 << len(reaches) < n_z // 2:
        reaches.append(2 << len(reaches))

    def greet(level):
        for i in (reaches[level], n_z - reaches[level]):
            pl.semaphore_signal(
                chain.at[level], inc=1, device_id=z_peers[i - 1], device_id_type=MESH
            )

    if reaches:
        greet(0)
    start_sum(0, halves)
    take_loads(1)
    halo_copies = []
    y_from = {-1: pl.ds(0, HALO), 0: pl.ds(0, rows_y), 1: pl.ds(rows_y - HALO, HALO)}
    y_to = {-1: pl.ds(rows_y, HALO), 0: pl.ds(0, rows_y), 1: pl.ds(rows_y + HALO, HALO)}

    def x_rows(ex, depth):
        if ex == 0:
            return 0, HALO, rows_x
        if ex == 1:
            return rows_x - depth, HALO - depth, depth
        return 0, HALO + rows_x, depth

    def send_sides(src, ext, depth, base, first_phase):
        for n, ((ex, ey), who) in enumerate(sides):
            if (ey == 0) != first_phase:
                continue
            first, to, count = x_rows(ex, depth - (1 if ex and ey else 0))
            halo_copies.append(
                remote(src.at[pl.ds(first, count), y_from[ey], :],
                       ext.at[pl.ds(to, count), y_to[ey], :],
                       halo_send.at[base + n], halo_recv.at[base + n], who)
            )
            ends.append(halo_copies[-1].wait_send)

    send_sides(diagonal_ref, ext_d, HALO - 1, 0, True)
    send_sides(source_ref, ext_s, HALO - 1, 8, True)
    for level in range(len(reaches)):
        pl.semaphore_wait(chain.at[level], 2)
        if level + 1 < len(reaches):
            greet(level + 1)
    middle_sum(0)
    n_rank = 0
    for (ex, ey), who in sides:
        if not (ex and ey):
            halo_copies.append(
                remote(ranks, ranks_in.at[n_rank],
                       halo_send.at[24 + n_rank], halo_recv.at[24 + n_rank], who)
            )
            ends.append(halo_copies[-1].wait_send)
            n_rank += 1
    send_sides(diagonal_ref, ext_d, HALO - 1, 0, False)
    send_sides(source_ref, ext_s, HALO - 1, 8, False)
    ext_d[pl.ds(HALO, rows_x), pl.ds(0, rows_y), :] = diagonal_ref[...]
    ext_s[pl.ds(HALO, rows_x), pl.ds(0, rows_y), :] = source_ref[...]

    take_loads(5)
    for n, part in enumerate(split3(inverse_ref[...])):
        inverse_parts[n] = part

    def pack(at, carry):
        for kt in range(k_all // 8):
            packed[kt, at] = rows_k[pl.ds(kt * 8 * per_k + at, 8, stride=per_k), :]
        return carry

    lax.fori_loop(0, per_k, pack, 0)

    for copy in halo_copies:
        copy.wait_recv()
    far = -100.0
    x_after = jnp.where(gx == n_gx - 1, far, ranks_in[0, 1])
    y_after = jnp.where(gy == n_gy - 1, far, ranks_in[1, 0])
    y_before = jnp.where(gy == 0, far, ranks_in[2, 0])
    x_before = jnp.where(gx == 0, far, ranks_in[3, 1])
    rank_x = []
    for rows in (x_before, own_x, x_after):
        for x in range(rows_x):
            rank_x.append(jnp.broadcast_to(rows[x : x + 1], tile))
    halo_y = jnp.where(sub < HALO, y_after, y_before)
    rank_y = jnp.concatenate([own_y, halo_y], axis=0)
    wide = (2 * rows_y, cells_z)
    n_ext = rows_x + 2 * HALO

    def widen(column):
        return jnp.concatenate([column] * (cells_z // LANES), axis=-1)

    def widen_x(rows):
        rows = widen(rows)
        return jnp.concatenate([rows, rows], axis=0)

    rank_y_wide = widen(rank_y)
    rank_x_wide = [widen_x(rows) for rows in rank_x]
    for r in range(1, n_ext - 1):
        here = (rank_x_wide[r] >= 0.0) & (rank_y_wide >= 0.0)
        w = jnp.where(here, TWO_THIRDS / (6.0 + ext_d[r]), 0.0)
        weight[r] = w
        weighted_q[r] = jnp.where(here, w * ext_s[r], 0.0)

    y_up = pltpu.roll(rank_y, 2 * rows_y - 1, 0)[:rows_y]
    y_down = pltpu.roll(rank_y, 1, 0)[:rows_y]

    def beside(x):
        r = HALO + x
        ranks_of = [
            rank_x[r - 1] * XY_CUTS + own_y,
            rank_x[r + 1] * XY_CUTS + own_y,
            rank_x[r] * XY_CUTS + y_up,
            rank_x[r] * XY_CUTS + y_down,
        ]

        def count(cell):
            cell = cell.astype(f32)
            return sum(jnp.where(rank == cell, 1.0, 0.0) for rank in ranks_of)

        return count

    z_lane = iota(wide, 1)

    def z_pair(values, z_lane):
        before = jnp.where(z_lane == 0, 0.0, pltpu.roll(values, 1, 1))
        after = jnp.where(z_lane == cells_z - 1, 0.0, pltpu.roll(values, cells_z - 1, 1))
        return before + after

    def correct(rhs, store):
        line = jnp.concatenate([rhs[0:1], rhs[1:2]], axis=1)
        at = iota((8, coarse), 0)
        left = jnp.zeros((8, coarse), f32)
        for n, part in enumerate(split3(line)):
            left = jnp.where(at == n, part.astype(f32), left)
        left = left.astype(bf16)
        solved = dot(left, inverse_parts[0], NT)
        solved = solved + jnp.where(at < 2, dot(left, inverse_parts[1], NT), 0.0)
        solved = solved + jnp.where(at < 1, dot(left, inverse_parts[2], NT), 0.0)
        solved = jnp.sum(solved, axis=0, keepdims=True)
        pairs = XY_CUTS * XY_CUTS
        row = iota((pairs, coarse), 0)
        column = iota((pairs, coarse), 1)
        spread = jnp.where(
            column // Z_CUTS == row, jnp.broadcast_to(solved, (pairs, coarse)), 0.0
        )
        parts = dot(jnp.concatenate(split3(spread), axis=0), map_g[...], NN)
        boxes = parts[:pairs] + parts[pairs : 2 * pairs] + parts[2 * pairs :]
        by_x = []
        for a in range(XY_CUTS):
            picked = jnp.zeros(wide, f32)
            for b in range(XY_CUTS):
                line = boxes[a * XY_CUTS + b : a * XY_CUTS + b + 1]
                picked = jnp.where(rank_y_wide == float(b), jnp.broadcast_to(line, wide), picked)
            by_x.append(picked)
        for r in range(n_ext):
            picked = jnp.zeros(wide, f32)
            for a in range(XY_CUTS):
                picked = jnp.where(rank_x_wide[r] == float(a), by_x[a], picked)
            store(r, picked)

    def sweep(old, new, r):
        here = old[r]
        around = old[r - 1] + old[r + 1]
        around = around + pltpu.roll(here, 1, 0) + pltpu.roll(here, 2 * rows_y - 1, 0)
        around = around + z_pair(here, z_lane)
        new[r] = here * THIRD + weighted_q[r] + weight[r] * around

    def smooth(last):
        fields = (field_a, field_b)
        for s in range(SWEEPS):
            for r in range(1 + s, n_ext - 1 - s):
                if s == SWEEPS - 1:
                    last(r, fields[s % 2])
                else:
                    sweep(fields[s % 2], fields[1 - s % 2], r)

    own_lane = iota((rows_y, cells_z), 1)

    def last_value(r, old):
        here = old[r]
        around = old[r - 1, pl.ds(0, rows_y), :] + old[r + 1, pl.ds(0, rows_y), :]
        beside_y = pltpu.roll(here, 1, 0) + pltpu.roll(here, 2 * rows_y - 1, 0)
        here = here[:rows_y]
        around = around + beside_y[:rows_y] + z_pair(here, own_lane)
        own = pl.ds(0, rows_y)
        return here * THIRD + weighted_q[r, own, :] + weight[r, own, :] * around

    def store_first(r, picked):
        field_a[r] = picked

    rhs = end_sum(0)
    correct(rhs, store_first)

    def last_first(r, old):
        ext_p[r, pl.ds(0, rows_y), :] = last_value(r, old)

    smooth(last_first)

    terms, stack = [], []
    for x in range(rows_x):
        p = ext_p[HALO + x, pl.ds(0, rows_y), :]
        stack.append(source_ref[x] - (6.0 + diagonal_ref[x]) * p + z_pair(p, own_lane))
    for x in range(rows_x):
        stack.append(ext_p[HALO + x, pl.ds(0, rows_y), :])
    values = along_z(jnp.concatenate(stack, axis=0))
    for x in range(2 * rows_x):
        count = same(box[x]) if x < rows_x else beside(x - rows_x)
        terms.append((values[x * rows_y : (x + 1) * rows_y], count))
    halves = to_boxes(terms)
    start_sum(1, halves)
    pressure_copies = len(halo_copies)
    own_p = ext_p.at[pl.ds(HALO, rows_x), pl.ds(0, rows_y), :]
    send_sides(own_p, ext_p, HALO, 16, True)

    middle_sum(1)
    send_sides(own_p, ext_p, HALO, 16, False)
    for copy in halo_copies[pressure_copies:]:
        copy.wait_recv()

    def store_second(r, picked):
        here = (rank_x_wide[r] >= 0.0) & (rank_y_wide >= 0.0)
        field_a[r] = picked + jnp.where(here, ext_p[r], 0.0)

    rhs = end_sum(1)
    correct(rhs, store_second)

    def last_second(r, old):
        final[pl.ds((r - HALO) * rows_y, rows_y), :] = last_value(r, old)

    smooth(last_second)

    n_far = n_grp // 2
    own_cells = pl.ds(pl.multiple_of(grp * per_k, per_k), per_k)
    pair_at = lax.div(grp, n_far) * n_far
    far_at = n_far - pair_at
    core_at = grp - pair_at
    others = [(0, far_at + lax.rem(core_at + i, n_far)) for i in range(n_far)]
    others += [(1, pair_at + lax.rem(core_at + i, n_far)) for i in range(1, n_far)]
    for n, (near_by, other) in enumerate(others):
        lanes = pl.ds(pl.multiple_of(other * LANES, LANES), LANES)
        copy = remote(final.at[:, lanes], snap.at[own_cells],
                      snap_send.at[n], snap_recv.at[near_by], (other, gx, gy))
        ends.append(copy.wait_send)
    own_lanes = pl.ds(pl.multiple_of(grp * LANES, LANES), LANES)
    snap[own_cells, :] = final[:, own_lanes]

    def products(base):
        def step(at, carry):
            rows = [
                jnp.broadcast_to(snap[pl.ds((base + t) * per_k + at, 1), :], (8, LANES))
                for t in range(n_far)
            ]
            out = []
            for kt in range(k_all // 8):
                taken = packed[kt, at]
                for t in range(n_far):
                    out.append(carry[kt * n_far + t] + taken * rows[t])
            return tuple(out)

        zeros = tuple(jnp.zeros((8, LANES), f32) for _ in range(k_all // 8 * n_far))
        sums = lax.fori_loop(0, per_k, step, zeros)
        for kt in range(k_all // 8):
            for t in range(n_far):
                to = pl.multiple_of((base + t) * k_all, 8) + kt * 8
                reduced[pl.ds(to, 8), :] = sums[kt * n_far + t]

    wait_bytes(snap.at[pl.ds(0, (n_far - 1) * per_k)], snap_recv.at[1])
    products(pair_at)
    wait_bytes(snap.at[pl.ds(0, n_far * per_k)], snap_recv.at[0])
    products(far_at)
    ones = jnp.ones((16, LANES), bf16)
    sums = sum(dot(ones, part, NT)[0:1] for part in split3(reduced[...]))
    n_out = n_grp * k_all
    for i in range(n_out // LANES):
        out_send[0, pl.ds(i, 1), :] = sums[:, i * LANES : (i + 1) * LANES]
    for i in range(n_out // LANES, 4):
        out_send[0, pl.ds(i, 1), :] = jnp.zeros((1, LANES), f32)
    all_at = grp * n_plane + plane_at
    pout[all_at] = out_send[0]
    for _, who in plane:
        remote(out_send.at[0], pout.at[all_at], sum_send_sem.at[2, 0], sum_recv_sem.at[2, 0], who)
    n_all = n_grp * n_plane
    ends.append(lambda: wait_bytes(pout.at[pl.ds(0, n_all - 1)], sum_send_sem.at[2, 0]))

    take_loads(2)

    def add_range(k, carry):
        total = range_in[k]
        for t in range(n_grp):
            total = total + omega_ref[t, k] * snap[pl.ds(t * per_k, per_k), :]
        range_done[k] = total
        return carry

    lax.fori_loop(0, range_in.shape[0], add_range, 0)

    wait_bytes(pout.at[pl.ds(0, n_all - 1)], sum_recv_sem.at[2, 0])
    total = pout[0]
    for i in range(1, n_all):
        total = total + pout[i]
    out_send[1] = total
    zout[z_at] = out_send[1]
    for who in far_first:
        remote(out_send.at[1], zout.at[z_at], sum_send_sem.at[2, 1], sum_recv_sem.at[2, 1], who)

    n_core = xi_ref.shape[1]
    by_t = iota((n_out, n_core), 0) // k_all
    columns = jnp.zeros((n_out, n_core), f32)
    for t in range(n_grp):
        line = jnp.broadcast_to(xi_ref[pl.ds(t, 1), :], (n_out, n_core))
        columns = jnp.where(by_t == t, line, columns)
    row_pick = iota((n_out, n_core), 0) % k_all == iota((n_out, n_core), 1)
    right = [part.astype(f32) for part in split3(columns)]
    right.append(jnp.where(row_pick, 1.0, 0.0))
    right = jnp.concatenate(right, axis=1).astype(bf16)
    core_pick = iota((k_phi, n_out), 1) % k_all == iota((k_phi, n_out), 0) + k_psi
    t_pick = iota((16, n_out), 1) // k_all == iota((16, n_out), 0)
    for end in ends:
        end()
    ends = [lambda: wait_bytes(zout.at[pl.ds(0, n_z - 1)], sum_send_sem.at[2, 1])]

    wait_bytes(zout.at[pl.ds(0, n_z - 1)], sum_recv_sem.at[2, 1])
    total = zout[0]
    for i in range(1, n_z):
        total = total + zout[i]
    line = jnp.concatenate([total[i : i + 1] for i in range(n_out // LANES)], axis=1)
    left = []
    for part in split3(line):
        part = part.astype(f32)
        left.append(jnp.where(core_pick, jnp.broadcast_to(part, (k_phi, n_out)), 0.0))
        left.append(jnp.where(t_pick, jnp.broadcast_to(part, (16, n_out)), 0.0))
    parts = dot(jnp.concatenate(left, axis=0).astype(bf16), right, NN)
    n = k_phi + 16
    result = parts[:n] + parts[n : 2 * n] + parts[2 * n :]
    images = result[:k_phi]
    core_sum = images[:, :n_core] + images[:, n_core : 2 * n_core] + images[:, 2 * n_core : 3 * n_core]
    core_out[...] = core_ref[...] + core_sum
    corange_out[...] = result[k_phi : k_phi + n_grp, 3 * n_core : 3 * n_core + k_psi]

    for end in ends:
        end()


def finish(range_in, corange_in, core_in, range_out, corange_out, core_out, sems):
    pairs = ((range_in, range_out), (corange_in, corange_out), (core_in, core_out))
    stores = [pltpu.make_async_copy(src, dst, sems.at[n]) for n, (src, dst) in enumerate(pairs)]
    for store in stores:
        store.start()
    for store in stores:
        store.wait()


def solution(mesh):
    n_grp, n_gx, n_gy = (mesh.shape[name] for name in ("grp", "gx", "gy"))
    n_z = min(16, n_gx // 2)
    n_low = n_gx // n_z

    def body(
        sources,
        diagonal,
        coarse_ids,
        coarse_inverse,
        omega_rows,
        psi,
        phi,
        xi_cols,
        range_sketch,
        core_sketch,
    ):
        _, rows_x, rows_y, cells_z = sources.shape
        total_cells = rows_x * n_gx * rows_y * n_gy * cells_z
        k_psi, k_phi = psi.shape[0], phi.shape[0]
        k_all = k_psi + k_phi
        k_range = range_sketch.shape[0]
        n_ext = rows_x + 2 * HALO
        per_k = rows_x * rows_y
        coarse = coarse_inverse.shape[0]
        vmem = pl.BlockSpec(memory_space=pltpu.VMEM)
        hbm = pl.BlockSpec(memory_space=pl.ANY)
        ext = pltpu.VMEM((n_ext, 2 * rows_y, cells_z), f32)
        call = pl.pallas_call(
            functools.partial(kernel, (n_grp, n_gx, n_gy, n_z, total_cells)),
            out_shape=(
                pltpu.VMEM((k_range, per_k, LANES), f32),
                pltpu.VMEM((n_grp, k_psi), f32),
                pltpu.VMEM(core_sketch.shape, f32),
            ),
            in_specs=[hbm] * 10,
            out_specs=(vmem, vmem, vmem),
            scratch_shapes=[
                pltpu.VMEM((rows_x, rows_y, cells_z), f32),
                pltpu.VMEM((rows_x, rows_y, cells_z), f32),
                pltpu.VMEM((rows_x, rows_y, cells_z), jnp.int32),
                pltpu.VMEM(coarse_inverse.shape, f32),
                pltpu.SMEM(omega_rows.shape, f32),
                pltpu.VMEM((n_grp, xi_cols.shape[0]), f32),
                pltpu.VMEM(core_sketch.shape, f32),
                pltpu.VMEM((k_all * per_k, LANES), f32),
                pltpu.VMEM((k_range, per_k, LANES), f32),
                ext,
                ext,
                ext,
                ext,
                ext,
                ext,
                ext,
                pltpu.VMEM((per_k, cells_z), f32),
                pltpu.VMEM((n_grp * per_k, LANES), f32),
                pltpu.VMEM((k_all // 8, per_k, 8, LANES), f32),
                pltpu.VMEM((n_grp * k_all, LANES), f32),
                pltpu.VMEM((2, rows_y, LANES), f32),
                pltpu.VMEM((4, 2, rows_y, LANES), f32),
                pltpu.VMEM((LANES, cells_z), bf16),
                pltpu.VMEM((coarse, cells_z), bf16),
                pltpu.VMEM((2, 2, 2, LANES), f32),
                pltpu.VMEM((2, n_z, 2, LANES), f32),
                pltpu.VMEM((2, n_low * n_gy, 2, LANES), f32),
                pltpu.VMEM((2, 4, LANES), f32),
                pltpu.VMEM((n_z, 4, LANES), f32),
                pltpu.VMEM((n_grp * n_low * n_gy, 4, LANES), f32),
                pltpu.SemaphoreType.DMA((10,)),
                pltpu.SemaphoreType.DMA((28,)),
                pltpu.SemaphoreType.DMA((28,)),
                pltpu.SemaphoreType.DMA((3, 2)),
                pltpu.SemaphoreType.DMA((3, 2)),
                pltpu.SemaphoreType.DMA((n_grp - 1,)),
                pltpu.SemaphoreType.DMA((2,)),
                pltpu.SemaphoreType.REGULAR((2,)),
                pltpu.VMEM((3, coarse, coarse), bf16),
            ],
            compiler_params=pltpu.CompilerParams(
                collective_id=0, has_side_effects=True
            ),
            name="two_level_sketch",
        )
        range_new, corange_cols, core_new = call(
            sources[0],
            diagonal,
            coarse_ids,
            coarse_inverse,
            omega_rows,
            psi.reshape(k_psi * per_k, LANES),
            phi.reshape(k_phi * per_k, LANES),
            xi_cols.T,
            range_sketch.reshape(k_range, per_k, LANES),
            core_sketch,
        )
        range_new, corange_cols, core_new = pl.pallas_call(
            finish,
            out_shape=(
                jax.ShapeDtypeStruct((k_range, per_k, LANES), f32),
                jax.ShapeDtypeStruct((n_grp, k_psi), f32),
                jax.ShapeDtypeStruct(core_sketch.shape, f32),
            ),
            in_specs=[vmem] * 3,
            out_specs=(hbm, hbm, hbm),
            scratch_shapes=[pltpu.SemaphoreType.DMA((3,))],
            compiler_params=pltpu.CompilerParams(vmem_limit_bytes=1 << 21),
            name="finish",
        )(range_new, corange_cols, core_new)
        return range_new.reshape(range_sketch.shape), corange_cols.T, core_new

    return jax.shard_map(
        body,
        mesh=mesh,
        in_specs=(
            P("grp", "gx", "gy", None),
            P("gx", "gy", None),
            P("gx", "gy", None),
            P(),
            P(),
            P(None, "gx", "gy", "grp"),
            P(None, "gx", "gy", "grp"),
            P(),
            P(None, "gx", "gy", "grp"),
            P(),
        ),
        out_specs=(P(None, "gx", "gy", "grp"), P(), P()),
        check_vma=False,
    )
```

```python
import functools

import jax
import jax.numpy as jnp
from jax import lax
from jax.experimental import pallas as pl
from jax.experimental.pallas import tpu as pltpu
from jax.sharding import PartitionSpec as P

OUTER = 2
SWEEPS = 4
XY_CUTS = 4
Z_CUTS = 16
HALO = 4
LANES = 128
THIRD = 1.0 / 3.0
TWO_THIRDS = 2.0 / 3.0

f32 = jnp.float32
bf16 = jnp.bfloat16
MESH = pl.DeviceIdType.MESH
HIGHEST = lax.Precision.HIGHEST
NT = (((1,), (1,)), ((), ()))
NN = (((1,), (0,)), ((), ()))


def dot(a, b, dims, precision=None):
    return lax.dot_general(a, b, dims, precision=precision, preferred_element_type=f32)


def split3(x):
    high = x.astype(bf16)
    rest = x - high.astype(f32)
    middle = rest.astype(bf16)
    low = (rest - middle.astype(f32)).astype(bf16)
    return high, middle, low


def iota(shape, dim):
    return lax.broadcasted_iota(jnp.int32, shape, dim)


def kernel(
    sizes,
    source_hbm,
    diagonal_hbm,
    ids_hbm,
    inverse_hbm,
    omega_hbm,
    psi_hbm,
    phi_hbm,
    xi_hbm,
    range_hbm,
    core_hbm,
    range_done,
    corange_out,
    core_out,
    source_ref,
    diagonal_ref,
    ids_ref,
    inverse_ref,
    omega_ref,
    xi_ref,
    core_ref,
    rows_k,
    range_in,
    ext_s,
    ext_d,
    ext_p,
    weight,
    weighted_q,
    field_a,
    field_b,
    final,
    snap,
    packed,
    reduced,
    ranks,
    ranks_in,
    map_zt,
    map_g,
    sum_send,
    zsum,
    psum,
    out_send,
    zout,
    pout,
    local_sem,
    halo_send,
    halo_recv,
    sum_send_sem,
    sum_recv_sem,
    snap_send,
    snap_recv,
    chain,
    inverse_parts,
    pair_send,
):
    n_grp, n_gx, n_gy, n_z, total_cells = sizes
    n_low = n_gx // n_z
    rows_x, rows_y, cells_z = source_ref.shape
    per_k = rows_x * rows_y
    k_psi, k_phi = psi_hbm.shape[0] // per_k, phi_hbm.shape[0] // per_k
    k_all = k_psi + k_phi
    coarse = inverse_ref.shape[0]
    grp, gx, gy = lax.axis_index("grp"), lax.axis_index("gx"), lax.axis_index("gy")
    z_at = lax.rem(gx, n_z)
    low_at = lax.div(gx, n_z)

    z_peers = [
        (grp, low_at * n_z + lax.rem(z_at + i, n_z), gy) for i in range(1, n_z)
    ]
    plane = []
    for i in range(n_grp):
        for j in range(n_low):
            for k in range(n_gy):
                if i or j or k:
                    who = (
                        lax.rem(grp + i, n_grp),
                        lax.rem(gx + j * n_z, n_gx),
                        lax.rem(gy + k, n_gy),
                    )
                    plane.append(((i, j, k), who))
    plane.sort(key=lambda peer: -(min(peer[0][0], n_grp - peer[0][0]) + peer[0][1]
                                  + min(peer[0][2], n_gy - peer[0][2])))
    own_plane = [who for (i, j, k), who in plane if i == 0]
    z_order = sorted(range(n_z - 1), key=lambda i: -min(i + 1, n_z - 1 - i))
    far_first = [z_peers[i] for i in z_order]
    sides = []
    for ex in (-1, 0, 1):
        for ey in (-1, 0, 1):
            if ex or ey:
                who = (grp, lax.rem(gx + ex + n_gx, n_gx), lax.rem(gy + ey + n_gy, n_gy))
                sides.append(((ex, ey), who))
    grp_peers = [who for (i, j, k), who in plane if j == 0 and k == 0]
    near_z = [z_peers[i - 1] for i in range(1, n_z) if min(i, n_z - i) <= 3]
    near = own_plane + near_z + [who for (_, ey), who in sides if ey == 0] + grp_peers
    pairs = (
        (ids_hbm, ids_ref),
        (source_hbm, source_ref),
        (diagonal_hbm, diagonal_ref),
        (inverse_hbm, inverse_ref),
        (xi_hbm, xi_ref),
        (omega_hbm, omega_ref),
        (psi_hbm, rows_k.at[pl.ds(0, k_psi * per_k)]),
        (phi_hbm, rows_k.at[pl.ds(k_psi * per_k, k_phi * per_k)]),
        (range_hbm, range_in),
        (core_hbm, core_ref),
    )
    loads = [
        pltpu.make_async_copy(src, dst, local_sem.at[n]) for n, (src, dst) in enumerate(pairs)
    ]
    for load in loads[:2]:
        load.start()
    barrier = pltpu.get_barrier_semaphore()
    for who in near:
        pl.semaphore_signal(barrier, inc=1, device_id=who, device_id_type=MESH)
    for load in loads[2:]:
        load.start()

    def remote(src, dst, send, recv, who):
        copy = pltpu.make_async_remote_copy(
            src_ref=src, dst_ref=dst, send_sem=send, recv_sem=recv,
            device_id=who, device_id_type=MESH,
        )
        copy.start()
        return copy

    ends = []

    def wait_bytes(ref, sem):
        pltpu.make_async_copy(ref, ref, sem).wait()

    def take_loads(count):
        for _ in range(count):
            loads.pop(0).wait()

    take_loads(1)

    tile = (rows_y, LANES)
    sub = iota(tile, 0)
    lane = iota(tile, 1)
    box_lane = lane // Z_CUTS
    box = [jnp.broadcast_to(ids_ref[x, :, 0:1] // Z_CUTS, tile) for x in range(rows_x)]
    own_y = (box[0] % XY_CUTS).astype(f32)
    own_x = jnp.zeros(tile, f32)
    for x in range(rows_x):
        own_x = jnp.where(sub == x, (box[x] // XY_CUTS).astype(f32), own_x)
    ranks[0] = own_y
    ranks[1] = own_x
    rank_z = ids_ref[0, 0:1, :] % Z_CUTS
    map_zt[...] = jnp.where(
        iota((LANES, cells_z), 0) % Z_CUTS == rank_z, 1.0, 0.0
    ).astype(bf16)
    map_g[...] = jnp.where(
        iota((coarse, cells_z), 0) % Z_CUTS == rank_z, 1.0, 0.0
    ).astype(bf16)

    def along_z(values):
        parts = dot(jnp.concatenate(split3(values), axis=0), map_zt[...], NT)
        n = values.shape[0]
        return parts[:n] + parts[n : 2 * n] + parts[2 * n :]

    def to_boxes(terms):
        halves = []
        for first in (0, LANES // Z_CUTS):
            total = jnp.zeros(tile, f32)
            for rows, count in terms:
                total = total + rows * count(box_lane + first)
            halves.append(jnp.sum(total, axis=0, keepdims=True))
        return halves

    def same(rank):
        return lambda cell: jnp.where(rank == cell, 1.0, 0.0)

    plane_at = low_at * n_gy + gy
    n_plane = n_low * n_gy

    def start_sum(which, halves):
        for i in range(2):
            sum_send[which, 0, pl.ds(i, 1), :] = halves[i]
        psum[which, plane_at] = sum_send[which, 0]
        for who in own_plane:
            remote(sum_send.at[which, 0], psum.at[which, plane_at],
                   sum_send_sem.at[which, 0], sum_recv_sem.at[which, 0], who)
        ends.append(lambda: wait_bytes(psum.at[which, pl.ds(0, n_plane - 1)], sum_send_sem.at[which, 0]))

    def middle_sum(which):
        wait_bytes(psum.at[which, pl.ds(0, n_plane - 1)], sum_recv_sem.at[which, 0])
        total = psum[which, 0]
        for i in range(1, n_plane):
            total = total + psum[which, i]
        sum_send[which, 1] = total
        zsum[which, z_at] = sum_send[which, 1]
        for who in far_first:
            remote(sum_send.at[which, 1], zsum.at[which, z_at],
                   sum_send_sem.at[which, 1], sum_recv_sem.at[which, 1], who)
        ends.append(lambda: wait_bytes(zsum.at[which, pl.ds(0, n_z - 1)], sum_send_sem.at[which, 1]))

    def end_sum(which):
        wait_bytes(zsum.at[which, pl.ds(0, n_z - 1)], sum_recv_sem.at[which, 1])
        total = zsum[which, 0]
        for i in range(1, n_z):
            total = total + zsum[which, i]
        return total * (coarse / total_cells)

    take_loads(1)

    values = along_z(source_ref[...].reshape(per_k, cells_z))
    first_terms = [
        (values[x * rows_y : (x + 1) * rows_y], same(box[x])) for x in range(rows_x)
    ]
    halves = to_boxes(first_terms)

    pl.semaphore_wait(barrier, len(near))
    reaches, known = [], 3
    while known < n_z // 2:
        reaches.append(min(3, n_z // 2 - known))
        known += reaches[-1]

    def greet(level):
        for i in (reaches[level], n_z - reaches[level]):
            pl.semaphore_signal(
                chain.at[level], inc=1, device_id=z_peers[i - 1], device_id_type=MESH
            )

    if reaches:
        greet(0)
    start_sum(0, halves)
    take_loads(1)
    halo_copies = []
    y_from = {-1: pl.ds(0, HALO), 0: pl.ds(0, rows_y), 1: pl.ds(rows_y - HALO, HALO)}
    y_to = {-1: pl.ds(rows_y, HALO), 0: pl.ds(0, rows_y), 1: pl.ds(rows_y + HALO, HALO)}

    def x_rows(ex, depth):
        if ex == 0:
            return 0, HALO, rows_x
        if ex == 1:
            return rows_x - depth, HALO - depth, depth
        return 0, HALO + rows_x, depth

    def send_sides(src, ext, depth, base, first_phase):
        for n, ((ex, ey), who) in enumerate(sides):
            if (ey == 0) != first_phase:
                continue
            first, to, count = x_rows(ex, depth - (1 if ex and ey else 0))
            halo_copies.append(
                remote(src.at[pl.ds(first, count), y_from[ey], :],
                       ext.at[pl.ds(to, count), y_to[ey], :],
                       halo_send.at[base + n], halo_recv.at[base + n], who)
            )
            ends.append(halo_copies[-1].wait_send)

    send_sides(diagonal_ref, ext_d, HALO - 1, 0, True)
    send_sides(source_ref, ext_s, HALO - 1, 8, True)
    for level in range(len(reaches)):
        pl.semaphore_wait(chain.at[level], 2)
        if level + 1 < len(reaches):
            greet(level + 1)
    middle_sum(0)
    n_rank = 0
    for (ex, ey), who in sides:
        if not (ex and ey):
            halo_copies.append(
                remote(ranks, ranks_in.at[n_rank],
                       halo_send.at[24 + n_rank], halo_recv.at[24 + n_rank], who)
            )
            ends.append(halo_copies[-1].wait_send)
            n_rank += 1
    send_sides(diagonal_ref, ext_d, HALO - 1, 0, False)
    send_sides(source_ref, ext_s, HALO - 1, 8, False)
    ext_d[pl.ds(HALO, rows_x), pl.ds(0, rows_y), :] = diagonal_ref[...]
    ext_s[pl.ds(HALO, rows_x), pl.ds(0, rows_y), :] = source_ref[...]

    take_loads(5)
    for n, part in enumerate(split3(inverse_ref[...])):
        inverse_parts[n] = part

    def pack(at, carry):
        for kt in range(k_all // 8):
            packed[kt, at] = rows_k[pl.ds(kt * 8 * per_k + at, 8, stride=per_k), :]
        return carry

    lax.fori_loop(0, per_k, pack, 0)

    for copy in halo_copies:
        copy.wait_recv()
    far = -100.0
    x_after = jnp.where(gx == n_gx - 1, far, ranks_in[0, 1])
    y_after = jnp.where(gy == n_gy - 1, far, ranks_in[1, 0])
    y_before = jnp.where(gy == 0, far, ranks_in[2, 0])
    x_before = jnp.where(gx == 0, far, ranks_in[3, 1])
    rank_x = []
    for rows in (x_before, own_x, x_after):
        for x in range(rows_x):
            rank_x.append(jnp.broadcast_to(rows[x : x + 1], tile))
    halo_y = jnp.where(sub < HALO, y_after, y_before)
    rank_y = jnp.concatenate([own_y, halo_y], axis=0)
    wide = (2 * rows_y, cells_z)
    n_ext = rows_x + 2 * HALO

    def widen(column):
        return jnp.concatenate([column] * (cells_z // LANES), axis=-1)

    def widen_x(rows):
        rows = widen(rows)
        return jnp.concatenate([rows, rows], axis=0)

    rank_y_wide = widen(rank_y)
    rank_x_wide = [widen_x(rows) for rows in rank_x]
    for r in range(1, n_ext - 1):
        here = (rank_x_wide[r] >= 0.0) & (rank_y_wide >= 0.0)
        w = jnp.where(here, TWO_THIRDS / (6.0 + ext_d[r]), 0.0)
        weight[r] = w
        weighted_q[r] = jnp.where(here, w * ext_s[r], 0.0)

    y_up = pltpu.roll(rank_y, 2 * rows_y - 1, 0)[:rows_y]
    y_down = pltpu.roll(rank_y, 1, 0)[:rows_y]

    def beside(x):
        r = HALO + x
        ranks_of = [
            rank_x[r - 1] * XY_CUTS + own_y,
            rank_x[r + 1] * XY_CUTS + own_y,
            rank_x[r] * XY_CUTS + y_up,
            rank_x[r] * XY_CUTS + y_down,
        ]

        def count(cell):
            cell = cell.astype(f32)
            return sum(jnp.where(rank == cell, 1.0, 0.0) for rank in ranks_of)

        return count

    z_lane = iota(wide, 1)

    def z_pair(values, z_lane):
        before = jnp.where(z_lane == 0, 0.0, pltpu.roll(values, 1, 1))
        after = jnp.where(z_lane == cells_z - 1, 0.0, pltpu.roll(values, cells_z - 1, 1))
        return before + after

    def correct(rhs, store):
        line = jnp.concatenate([rhs[0:1], rhs[1:2]], axis=1)
        at = iota((8, coarse), 0)
        left = jnp.zeros((8, coarse), f32)
        for n, part in enumerate(split3(line)):
            left = jnp.where(at == n, part.astype(f32), left)
        left = left.astype(bf16)
        solved = dot(left, inverse_parts[0], NT)
        solved = solved + jnp.where(at < 2, dot(left, inverse_parts[1], NT), 0.0)
        solved = solved + jnp.where(at < 1, dot(left, inverse_parts[2], NT), 0.0)
        solved = jnp.sum(solved, axis=0, keepdims=True)
        pairs = XY_CUTS * XY_CUTS
        row = iota((pairs, coarse), 0)
        column = iota((pairs, coarse), 1)
        spread = jnp.where(
            column // Z_CUTS == row, jnp.broadcast_to(solved, (pairs, coarse)), 0.0
        )
        parts = dot(jnp.concatenate(split3(spread), axis=0), map_g[...], NN)
        boxes = parts[:pairs] + parts[pairs : 2 * pairs] + parts[2 * pairs :]
        by_x = []
        for a in range(XY_CUTS):
            picked = jnp.zeros(wide, f32)
            for b in range(XY_CUTS):
                line = boxes[a * XY_CUTS + b : a * XY_CUTS + b + 1]
                picked = jnp.where(rank_y_wide == float(b), jnp.broadcast_to(line, wide), picked)
            by_x.append(picked)
        for r in range(n_ext):
            picked = jnp.zeros(wide, f32)
            for a in range(XY_CUTS):
                picked = jnp.where(rank_x_wide[r] == float(a), by_x[a], picked)
            store(r, picked)

    def sweep(old, new, r):
        here = old[r]
        around = old[r - 1] + old[r + 1]
        around = around + pltpu.roll(here, 1, 0) + pltpu.roll(here, 2 * rows_y - 1, 0)
        around = around + z_pair(here, z_lane)
        new[r] = here * THIRD + weighted_q[r] + weight[r] * around

    def smooth(last):
        fields = (field_a, field_b)
        for s in range(SWEEPS):
            for r in range(1 + s, n_ext - 1 - s):
                if s == SWEEPS - 1:
                    last(r, fields[s % 2])
                else:
                    sweep(fields[s % 2], fields[1 - s % 2], r)

    own_lane = iota((rows_y, cells_z), 1)

    def last_value(r, old):
        here = old[r]
        around = old[r - 1, pl.ds(0, rows_y), :] + old[r + 1, pl.ds(0, rows_y), :]
        beside_y = pltpu.roll(here, 1, 0) + pltpu.roll(here, 2 * rows_y - 1, 0)
        here = here[:rows_y]
        around = around + beside_y[:rows_y] + z_pair(here, own_lane)
        own = pl.ds(0, rows_y)
        return here * THIRD + weighted_q[r, own, :] + weight[r, own, :] * around

    def store_first(r, picked):
        field_a[r] = picked

    rhs = end_sum(0)
    correct(rhs, store_first)

    def last_first(r, old):
        ext_p[r, pl.ds(0, rows_y), :] = last_value(r, old)

    smooth(last_first)

    terms, stack = [], []
    for x in range(rows_x):
        p = ext_p[HALO + x, pl.ds(0, rows_y), :]
        stack.append(source_ref[x] - (6.0 + diagonal_ref[x]) * p + z_pair(p, own_lane))
    for x in range(rows_x):
        stack.append(ext_p[HALO + x, pl.ds(0, rows_y), :])
    values = along_z(jnp.concatenate(stack, axis=0))
    for x in range(2 * rows_x):
        count = same(box[x]) if x < rows_x else beside(x - rows_x)
        terms.append((values[x * rows_y : (x + 1) * rows_y], count))
    halves = to_boxes(terms)
    start_sum(1, halves)
    pressure_copies = len(halo_copies)
    own_p = ext_p.at[pl.ds(HALO, rows_x), pl.ds(0, rows_y), :]
    send_sides(own_p, ext_p, HALO, 16, True)

    middle_sum(1)
    send_sides(own_p, ext_p, HALO, 16, False)
    for copy in halo_copies[pressure_copies:]:
        copy.wait_recv()

    def store_second(r, picked):
        here = (rank_x_wide[r] >= 0.0) & (rank_y_wide >= 0.0)
        field_a[r] = picked + jnp.where(here, ext_p[r], 0.0)

    rhs = end_sum(1)
    correct(rhs, store_second)

    def last_second(r, old):
        final[pl.ds((r - HALO) * rows_y, rows_y), :] = last_value(r, old)

    smooth(last_second)

    n_far = n_grp // 2
    own_cells = pl.ds(pl.multiple_of(grp * per_k, per_k), per_k)
    pair_at = lax.div(grp, n_far) * n_far
    far_at = n_far - pair_at
    core_at = grp - pair_at
    others = [(0, far_at + lax.rem(core_at + i, n_far)) for i in range(n_far)]
    others += [(1, pair_at + lax.rem(core_at + i, n_far)) for i in range(1, n_far)]
    for n, (near_by, other) in enumerate(others):
        lanes = pl.ds(pl.multiple_of(other * LANES, LANES), LANES)
        copy = remote(final.at[:, lanes], snap.at[own_cells],
                      snap_send.at[n], snap_recv.at[near_by], (other, gx, gy))
        ends.append(copy.wait_send)
    own_lanes = pl.ds(pl.multiple_of(grp * LANES, LANES), LANES)
    snap[own_cells, :] = final[:, own_lanes]

    def products(base):
        def step(at, carry):
            rows = [
                jnp.broadcast_to(snap[pl.ds((base + t) * per_k + at, 1), :], (8, LANES))
                for t in range(n_far)
            ]
            out = []
            for kt in range(k_all // 8):
                taken = packed[kt, at]
                for t in range(n_far):
                    out.append(carry[kt * n_far + t] + taken * rows[t])
            return tuple(out)

        zeros = tuple(jnp.zeros((8, LANES), f32) for _ in range(k_all // 8 * n_far))
        sums = lax.fori_loop(0, per_k, step, zeros)
        for kt in range(k_all // 8):
            for t in range(n_far):
                to = pl.multiple_of((base + t) * k_all, 8) + kt * 8
                reduced[pl.ds(to, 8), :] = sums[kt * n_far + t]

    wait_bytes(snap.at[pl.ds(0, (n_far - 1) * per_k)], snap_recv.at[1])
    products(pair_at)
    wait_bytes(snap.at[pl.ds(0, n_far * per_k)], snap_recv.at[0])
    products(far_at)
    ones = jnp.ones((16, LANES), bf16)
    sums = sum(dot(ones, part, NT)[0:1] for part in split3(reduced[...]))
    n_out = n_grp * k_all
    for i in range(n_out // LANES):
        out_send[0, pl.ds(i, 1), :] = sums[:, i * LANES : (i + 1) * LANES]
    for i in range(n_out // LANES, 4):
        out_send[0, pl.ds(i, 1), :] = jnp.zeros((1, LANES), f32)
    all_at = grp * n_plane + plane_at
    summing = core_at == n_far - 1
    partner = (grp + 1 - 2 * core_at, gx, gy)
    pair_index = lax.div(grp, n_far)
    chips = []
    for i in range(n_grp // n_far):
        for j in range(n_low):
            for k in range(n_gy):
                who = (
                    lax.rem(pair_index + i, n_grp // n_far) * n_far + n_far - 1,
                    lax.rem(gx + j * n_z, n_gx),
                    lax.rem(gy + k, n_gy),
                )
                chips.append((2 * i + j + min(k, n_gy - k), who))
    chips = [who for away, who in sorted(chips, key=lambda chip: -chip[0]) if away]
    pout[all_at] = out_send[0]
    for who in chips:
        remote(out_send.at[0], pout.at[all_at], sum_send_sem.at[2, 0], sum_recv_sem.at[2, 0], who)
    ends.append(lambda: wait_bytes(pout.at[pl.ds(0, len(chips))], sum_send_sem.at[2, 0]))

    @pl.when(jnp.logical_not(summing))
    def _():
        remote(out_send.at[0], pout.at[all_at], pair_send.at[0], sum_recv_sem.at[2, 0], partner)

    n_all = n_grp * n_plane

    take_loads(2)

    def add_range(k, carry):
        total = range_in[k]
        for t in range(n_grp):
            total = total + omega_ref[t, k] * snap[pl.ds(t * per_k, per_k), :]
        range_done[k] = total
        return carry

    lax.fori_loop(0, range_in.shape[0], add_range, 0)

    @pl.when(summing)
    def _():
        wait_bytes(pout.at[pl.ds(0, n_all - 1)], sum_recv_sem.at[2, 0])
        total = pout[0]
        for i in range(1, n_all):
            total = total + pout[i]
        out_send[1] = total
        zout[z_at] = out_send[1]
        for _, who_x, who_y in far_first:
            for who in ((partner[0], who_x, who_y), (grp, who_x, who_y)):
                remote(out_send.at[1], zout.at[z_at],
                       sum_send_sem.at[2, 1], sum_recv_sem.at[2, 1], who)
        remote(out_send.at[1], zout.at[z_at], sum_send_sem.at[2, 1], sum_recv_sem.at[2, 1], partner)

    n_core = xi_ref.shape[1]
    by_t = iota((n_out, n_core), 0) // k_all
    columns = jnp.zeros((n_out, n_core), f32)
    for t in range(n_grp):
        line = jnp.broadcast_to(xi_ref[pl.ds(t, 1), :], (n_out, n_core))
        columns = jnp.where(by_t == t, line, columns)
    row_pick = iota((n_out, n_core), 0) % k_all == iota((n_out, n_core), 1)
    right = [part.astype(f32) for part in split3(columns)]
    right.append(jnp.where(row_pick, 1.0, 0.0))
    right = jnp.concatenate(right, axis=1).astype(bf16)
    core_pick = iota((k_phi, n_out), 1) % k_all == iota((k_phi, n_out), 0) + k_psi
    t_pick = iota((16, n_out), 1) // k_all == iota((16, n_out), 0)
    for end in ends:
        end()

    @pl.when(summing)
    def _():
        wait_bytes(zout.at[pl.ds(0, n_z - 1)], sum_recv_sem.at[2, 1])

    @pl.when(jnp.logical_not(summing))
    def _():
        wait_bytes(zout, sum_recv_sem.at[2, 1])

    total = zout[0]
    for i in range(1, n_z):
        total = total + zout[i]
    line = jnp.concatenate([total[i : i + 1] for i in range(n_out // LANES)], axis=1)
    left = []
    for part in split3(line):
        part = part.astype(f32)
        left.append(jnp.where(core_pick, jnp.broadcast_to(part, (k_phi, n_out)), 0.0))
        left.append(jnp.where(t_pick, jnp.broadcast_to(part, (16, n_out)), 0.0))
    parts = dot(jnp.concatenate(left, axis=0).astype(bf16), right, NN)
    n = k_phi + 16
    result = parts[:n] + parts[n : 2 * n] + parts[2 * n :]
    images = result[:k_phi]
    core_sum = images[:, :n_core] + images[:, n_core : 2 * n_core] + images[:, 2 * n_core : 3 * n_core]
    core_out[...] = core_ref[...] + core_sum
    corange_out[...] = result[k_phi : k_phi + n_grp, 3 * n_core : 3 * n_core + k_psi]

    @pl.when(summing)
    def _():
        wait_bytes(pout.at[pl.ds(0, 2 * n_z - 1)], sum_send_sem.at[2, 1])

    @pl.when(jnp.logical_not(summing))
    def _():
        wait_bytes(pout.at[0], pair_send.at[0])


def finish(range_in, corange_in, core_in, range_out, corange_out, core_out, sems):
    pairs = ((range_in, range_out), (corange_in, corange_out), (core_in, core_out))
    stores = [pltpu.make_async_copy(src, dst, sems.at[n]) for n, (src, dst) in enumerate(pairs)]
    for store in stores:
        store.start()
    for store in stores:
        store.wait()


def solution(mesh):
    n_grp, n_gx, n_gy = (mesh.shape[name] for name in ("grp", "gx", "gy"))
    n_z = min(16, n_gx // 2)
    n_low = n_gx // n_z

    def body(
        sources,
        diagonal,
        coarse_ids,
        coarse_inverse,
        omega_rows,
        psi,
        phi,
        xi_cols,
        range_sketch,
        core_sketch,
    ):
        _, rows_x, rows_y, cells_z = sources.shape
        total_cells = rows_x * n_gx * rows_y * n_gy * cells_z
        k_psi, k_phi = psi.shape[0], phi.shape[0]
        k_all = k_psi + k_phi
        k_range = range_sketch.shape[0]
        n_ext = rows_x + 2 * HALO
        per_k = rows_x * rows_y
        coarse = coarse_inverse.shape[0]
        vmem = pl.BlockSpec(memory_space=pltpu.VMEM)
        hbm = pl.BlockSpec(memory_space=pl.ANY)
        ext = pltpu.VMEM((n_ext, 2 * rows_y, cells_z), f32)
        call = pl.pallas_call(
            functools.partial(kernel, (n_grp, n_gx, n_gy, n_z, total_cells)),
            out_shape=(
                pltpu.VMEM((k_range, per_k, LANES), f32),
                pltpu.VMEM((n_grp, k_psi), f32),
                pltpu.VMEM(core_sketch.shape, f32),
            ),
            in_specs=[hbm] * 10,
            out_specs=(vmem, vmem, vmem),
            scratch_shapes=[
                pltpu.VMEM((rows_x, rows_y, cells_z), f32),
                pltpu.VMEM((rows_x, rows_y, cells_z), f32),
                pltpu.VMEM((rows_x, rows_y, cells_z), jnp.int32),
                pltpu.VMEM(coarse_inverse.shape, f32),
                pltpu.SMEM(omega_rows.shape, f32),
                pltpu.VMEM((n_grp, xi_cols.shape[0]), f32),
                pltpu.VMEM(core_sketch.shape, f32),
                pltpu.VMEM((k_all * per_k, LANES), f32),
                pltpu.VMEM((k_range, per_k, LANES), f32),
                ext,
                ext,
                ext,
                ext,
                ext,
                ext,
                ext,
                pltpu.VMEM((per_k, cells_z), f32),
                pltpu.VMEM((n_grp * per_k, LANES), f32),
                pltpu.VMEM((k_all // 8, per_k, 8, LANES), f32),
                pltpu.VMEM((n_grp * k_all, LANES), f32),
                pltpu.VMEM((2, rows_y, LANES), f32),
                pltpu.VMEM((4, 2, rows_y, LANES), f32),
                pltpu.VMEM((LANES, cells_z), bf16),
                pltpu.VMEM((coarse, cells_z), bf16),
                pltpu.VMEM((2, 2, 2, LANES), f32),
                pltpu.VMEM((2, n_z, 2, LANES), f32),
                pltpu.VMEM((2, n_low * n_gy, 2, LANES), f32),
                pltpu.VMEM((2, 4, LANES), f32),
                pltpu.VMEM((n_z, 4, LANES), f32),
                pltpu.VMEM((n_grp * n_low * n_gy, 4, LANES), f32),
                pltpu.SemaphoreType.DMA((10,)),
                pltpu.SemaphoreType.DMA((28,)),
                pltpu.SemaphoreType.DMA((28,)),
                pltpu.SemaphoreType.DMA((3, 2)),
                pltpu.SemaphoreType.DMA((3, 2)),
                pltpu.SemaphoreType.DMA((n_grp - 1,)),
                pltpu.SemaphoreType.DMA((2,)),
                pltpu.SemaphoreType.REGULAR((2,)),
                pltpu.VMEM((3, coarse, coarse), bf16),
                pltpu.SemaphoreType.DMA((1,)),
            ],
            compiler_params=pltpu.CompilerParams(
                collective_id=0, has_side_effects=True
            ),
            name="two_level_sketch",
        )
        range_new, corange_cols, core_new = call(
            sources[0],
            diagonal,
            coarse_ids,
            coarse_inverse,
            omega_rows,
            psi.reshape(k_psi * per_k, LANES),
            phi.reshape(k_phi * per_k, LANES),
            xi_cols.T,
            range_sketch.reshape(k_range, per_k, LANES),
            core_sketch,
        )
        range_new, corange_cols, core_new = pl.pallas_call(
            finish,
            out_shape=(
                jax.ShapeDtypeStruct((k_range, per_k, LANES), f32),
                jax.ShapeDtypeStruct((n_grp, k_psi), f32),
                jax.ShapeDtypeStruct(core_sketch.shape, f32),
            ),
            in_specs=[vmem] * 3,
            out_specs=(hbm, hbm, hbm),
            scratch_shapes=[pltpu.SemaphoreType.DMA((3,))],
            compiler_params=pltpu.CompilerParams(vmem_limit_bytes=1 << 21),
            name="finish",
        )(range_new, corange_cols, core_new)
        return range_new.reshape(range_sketch.shape), corange_cols.T, core_new

    return jax.shard_map(
        body,
        mesh=mesh,
        in_specs=(
            P("grp", "gx", "gy", None),
            P("gx", "gy", None),
            P("gx", "gy", None),
            P(),
            P(),
            P(None, "gx", "gy", "grp"),
            P(None, "gx", "gy", "grp"),
            P(),
            P(None, "gx", "gy", "grp"),
            P(),
        ),
        out_specs=(P(None, "gx", "gy", "grp"), P(), P()),
        check_vma=False,
    )
```

```python
import functools

import jax
import jax.numpy as jnp
from jax import lax
from jax.experimental import pallas as pl
from jax.experimental.pallas import tpu as pltpu
from jax.sharding import PartitionSpec as P

OUTER = 2
SWEEPS = 4
XY_CUTS = 4
Z_CUTS = 16
HALO = 4
LANES = 128
THIRD = 1.0 / 3.0
TWO_THIRDS = 2.0 / 3.0

f32 = jnp.float32
bf16 = jnp.bfloat16
MESH = pl.DeviceIdType.MESH
HIGHEST = lax.Precision.HIGHEST
NT = (((1,), (1,)), ((), ()))
NN = (((1,), (0,)), ((), ()))


def dot(a, b, dims, precision=None):
    return lax.dot_general(a, b, dims, precision=precision, preferred_element_type=f32)


def split3(x):
    high = x.astype(bf16)
    rest = x - high.astype(f32)
    middle = rest.astype(bf16)
    low = (rest - middle.astype(f32)).astype(bf16)
    return high, middle, low


def iota(shape, dim):
    return lax.broadcasted_iota(jnp.int32, shape, dim)


def kernel(
    sizes,
    source_hbm,
    diagonal_hbm,
    ids_hbm,
    inverse_hbm,
    omega_hbm,
    psi_hbm,
    phi_hbm,
    xi_hbm,
    range_hbm,
    core_hbm,
    range_done,
    corange_out,
    core_out,
    source_ref,
    diagonal_ref,
    ids_ref,
    inverse_ref,
    omega_ref,
    xi_ref,
    core_ref,
    rows_k,
    range_in,
    ext_s,
    ext_d,
    ext_p,
    weight,
    weighted_q,
    field_a,
    field_b,
    final,
    snap,
    packed,
    reduced,
    ranks,
    ranks_in,
    map_zt,
    map_g,
    sum_send,
    zsum,
    psum,
    out_send,
    zout,
    pout,
    local_sem,
    halo_send,
    halo_recv,
    sum_send_sem,
    sum_recv_sem,
    snap_send,
    snap_recv,
    chain,
    inverse_parts,
    pair_send,
):
    n_grp, n_gx, n_gy, n_z, total_cells = sizes
    n_low = n_gx // n_z
    rows_x, rows_y, cells_z = source_ref.shape
    per_k = rows_x * rows_y
    k_psi, k_phi = psi_hbm.shape[0] // per_k, phi_hbm.shape[0] // per_k
    k_all = k_psi + k_phi
    coarse = inverse_ref.shape[0]
    grp, gx, gy = lax.axis_index("grp"), lax.axis_index("gx"), lax.axis_index("gy")
    z_at = lax.rem(gx, n_z)
    low_at = lax.div(gx, n_z)

    z_peers = [
        (grp, low_at * n_z + lax.rem(z_at + i, n_z), gy) for i in range(1, n_z)
    ]
    plane = []
    for i in range(n_grp):
        for j in range(n_low):
            for k in range(n_gy):
                if i or j or k:
                    who = (
                        lax.rem(grp + i, n_grp),
                        lax.rem(gx + j * n_z, n_gx),
                        lax.rem(gy + k, n_gy),
                    )
                    plane.append(((i, j, k), who))
    plane.sort(key=lambda peer: -(min(peer[0][0], n_grp - peer[0][0]) + peer[0][1]
                                  + min(peer[0][2], n_gy - peer[0][2])))
    own_plane = [who for (i, j, k), who in plane if i == 0]
    z_order = sorted(range(n_z - 1), key=lambda i: -min(i + 1, n_z - 1 - i))
    far_first = [z_peers[i] for i in z_order]
    sides = []
    for ex in (-1, 0, 1):
        for ey in (-1, 0, 1):
            if ex or ey:
                who = (grp, lax.rem(gx + ex + n_gx, n_gx), lax.rem(gy + ey + n_gy, n_gy))
                sides.append(((ex, ey), who))
    grp_peers = [who for (i, j, k), who in plane if j == 0 and k == 0]
    near_z = [z_peers[i - 1] for i in range(1, n_z) if min(i, n_z - i) <= 3]
    near = own_plane + near_z + [who for (_, ey), who in sides if ey == 0] + grp_peers
    pairs = (
        (ids_hbm, ids_ref),
        (source_hbm, source_ref),
        (diagonal_hbm, diagonal_ref),
        (inverse_hbm, inverse_ref),
        (xi_hbm, xi_ref),
        (omega_hbm, omega_ref),
        (psi_hbm, rows_k.at[pl.ds(0, k_psi * per_k)]),
        (phi_hbm, rows_k.at[pl.ds(k_psi * per_k, k_phi * per_k)]),
        (range_hbm, range_in),
        (core_hbm, core_ref),
    )
    loads = [
        pltpu.make_async_copy(src, dst, local_sem.at[n]) for n, (src, dst) in enumerate(pairs)
    ]
    for load in loads[:2]:
        load.start()
    barrier = pltpu.get_barrier_semaphore()
    for who in near:
        pl.semaphore_signal(barrier, inc=1, device_id=who, device_id_type=MESH)
    for load in loads[2:]:
        load.start()

    def remote(src, dst, send, recv, who):
        copy = pltpu.make_async_remote_copy(
            src_ref=src, dst_ref=dst, send_sem=send, recv_sem=recv,
            device_id=who, device_id_type=MESH,
        )
        copy.start()
        return copy

    ends = []

    def wait_bytes(ref, sem):
        pltpu.make_async_copy(ref, ref, sem).wait()

    def take_loads(count):
        for _ in range(count):
            loads.pop(0).wait()

    take_loads(1)

    tile = (rows_y, LANES)
    sub = iota(tile, 0)
    lane = iota(tile, 1)
    box_lane = lane // Z_CUTS
    box = [jnp.broadcast_to(ids_ref[x, :, 0:1] // Z_CUTS, tile) for x in range(rows_x)]
    own_y = (box[0] % XY_CUTS).astype(f32)
    own_x = jnp.zeros(tile, f32)
    for x in range(rows_x):
        own_x = jnp.where(sub == x, (box[x] // XY_CUTS).astype(f32), own_x)
    ranks[0] = own_y
    ranks[1] = own_x
    rank_z = ids_ref[0, 0:1, :] % Z_CUTS
    map_zt[...] = jnp.where(
        iota((LANES, cells_z), 0) % Z_CUTS == rank_z, 1.0, 0.0
    ).astype(bf16)
    map_g[...] = jnp.where(
        iota((coarse, cells_z), 0) % Z_CUTS == rank_z, 1.0, 0.0
    ).astype(bf16)

    def along_z(values):
        parts = dot(jnp.concatenate(split3(values), axis=0), map_zt[...], NT)
        n = values.shape[0]
        return parts[:n] + parts[n : 2 * n] + parts[2 * n :]

    def to_boxes(terms):
        halves = []
        for first in (0, LANES // Z_CUTS):
            total = jnp.zeros(tile, f32)
            for rows, count in terms:
                total = total + rows * count(box_lane + first)
            halves.append(jnp.sum(total, axis=0, keepdims=True))
        return halves

    def same(rank):
        return lambda cell: jnp.where(rank == cell, 1.0, 0.0)

    plane_at = low_at * n_gy + gy
    n_plane = n_low * n_gy

    def start_sum(which, halves):
        for i in range(2):
            sum_send[which, 0, pl.ds(i, 1), :] = halves[i]
        psum[which, plane_at] = sum_send[which, 0]
        for who in own_plane:
            remote(sum_send.at[which, 0], psum.at[which, plane_at],
                   sum_send_sem.at[which, 0], sum_recv_sem.at[which, 0], who)
        ends.append(lambda: wait_bytes(psum.at[which, pl.ds(0, n_plane - 1)], sum_send_sem.at[which, 0]))

    def middle_sum(which):
        wait_bytes(psum.at[which, pl.ds(0, n_plane - 1)], sum_recv_sem.at[which, 0])
        total = psum[which, 0]
        for i in range(1, n_plane):
            total = total + psum[which, i]
        sum_send[which, 1] = total
        zsum[which, z_at] = sum_send[which, 1]
        for who in far_first:
            remote(sum_send.at[which, 1], zsum.at[which, z_at],
                   sum_send_sem.at[which, 1], sum_recv_sem.at[which, 1], who)
        ends.append(lambda: wait_bytes(zsum.at[which, pl.ds(0, n_z - 1)], sum_send_sem.at[which, 1]))

    def end_sum(which):
        wait_bytes(zsum.at[which, pl.ds(0, n_z - 1)], sum_recv_sem.at[which, 1])
        total = zsum[which, 0]
        for i in range(1, n_z):
            total = total + zsum[which, i]
        return total * (coarse / total_cells)

    take_loads(1)

    values = along_z(source_ref[...].reshape(per_k, cells_z))
    first_terms = [
        (values[x * rows_y : (x + 1) * rows_y], same(box[x])) for x in range(rows_x)
    ]
    halves = to_boxes(first_terms)

    pl.semaphore_wait(barrier, len(near))
    reaches, known = [], 3
    while known < n_z // 2:
        reaches.append(min(3, n_z // 2 - known))
        known += reaches[-1]

    def greet(level):
        for i in (reaches[level], n_z - reaches[level]):
            pl.semaphore_signal(
                chain.at[level], inc=1, device_id=z_peers[i - 1], device_id_type=MESH
            )

    if reaches:
        greet(0)
    start_sum(0, halves)
    take_loads(1)
    halo_copies = []
    y_from = {-1: pl.ds(0, HALO), 0: pl.ds(0, rows_y), 1: pl.ds(rows_y - HALO, HALO)}
    y_to = {-1: pl.ds(rows_y, HALO), 0: pl.ds(0, rows_y), 1: pl.ds(rows_y + HALO, HALO)}

    def x_rows(ex, depth):
        if ex == 0:
            return 0, HALO, rows_x
        if ex == 1:
            return rows_x - depth, HALO - depth, depth
        return 0, HALO + rows_x, depth

    def send_sides(src, ext, depth, base, first_phase):
        for n, ((ex, ey), who) in enumerate(sides):
            if (ey == 0) != first_phase:
                continue
            first, to, count = x_rows(ex, depth - (1 if ex and ey else 0))
            halo_copies.append(
                remote(src.at[pl.ds(first, count), y_from[ey], :],
                       ext.at[pl.ds(to, count), y_to[ey], :],
                       halo_send.at[base + n], halo_recv.at[base + n], who)
            )
            ends.append(halo_copies[-1].wait_send)

    send_sides(diagonal_ref, ext_d, HALO - 1, 0, True)
    send_sides(source_ref, ext_s, HALO - 1, 8, True)
    for level in range(len(reaches)):
        pl.semaphore_wait(chain.at[level], 2)
        if level + 1 < len(reaches):
            greet(level + 1)
    middle_sum(0)
    n_rank = 0
    for (ex, ey), who in sides:
        if not (ex and ey):
            halo_copies.append(
                remote(ranks, ranks_in.at[n_rank],
                       halo_send.at[24 + n_rank], halo_recv.at[24 + n_rank], who)
            )
            ends.append(halo_copies[-1].wait_send)
            n_rank += 1
    send_sides(diagonal_ref, ext_d, HALO - 1, 0, False)
    send_sides(source_ref, ext_s, HALO - 1, 8, False)
    ext_d[pl.ds(HALO, rows_x), pl.ds(0, rows_y), :] = diagonal_ref[...]
    ext_s[pl.ds(HALO, rows_x), pl.ds(0, rows_y), :] = source_ref[...]

    take_loads(5)
    for n, part in enumerate(split3(inverse_ref[...])):
        inverse_parts[n] = part

    def pack(at, carry):
        for kt in range(k_all // 8):
            packed[kt, at] = rows_k[pl.ds(kt * 8 * per_k + at, 8, stride=per_k), :]
        return carry

    lax.fori_loop(0, per_k, pack, 0)

    for copy in halo_copies:
        copy.wait_recv()
    far = -100.0
    x_after = jnp.where(gx == n_gx - 1, far, ranks_in[0, 1])
    y_after = jnp.where(gy == n_gy - 1, far, ranks_in[1, 0])
    y_before = jnp.where(gy == 0, far, ranks_in[2, 0])
    x_before = jnp.where(gx == 0, far, ranks_in[3, 1])
    rank_x = []
    for rows in (x_before, own_x, x_after):
        for x in range(rows_x):
            rank_x.append(jnp.broadcast_to(rows[x : x + 1], tile))
    halo_y = jnp.where(sub < HALO, y_after, y_before)
    rank_y = jnp.concatenate([own_y, halo_y], axis=0)
    wide = (2 * rows_y, cells_z)
    n_ext = rows_x + 2 * HALO

    def widen(column):
        return jnp.concatenate([column] * (cells_z // LANES), axis=-1)

    def widen_x(rows):
        rows = widen(rows)
        return jnp.concatenate([rows, rows], axis=0)

    rank_y_wide = widen(rank_y)
    rank_x_wide = [widen_x(rows) for rows in rank_x]
    for r in range(1, n_ext - 1):
        here = (rank_x_wide[r] >= 0.0) & (rank_y_wide >= 0.0)
        w = jnp.where(here, TWO_THIRDS / (6.0 + ext_d[r]), 0.0)
        weight[r] = w
        weighted_q[r] = jnp.where(here, w * ext_s[r], 0.0)

    y_up = pltpu.roll(rank_y, 2 * rows_y - 1, 0)[:rows_y]
    y_down = pltpu.roll(rank_y, 1, 0)[:rows_y]

    def beside(x):
        r = HALO + x
        ranks_of = [
            rank_x[r - 1] * XY_CUTS + own_y,
            rank_x[r + 1] * XY_CUTS + own_y,
            rank_x[r] * XY_CUTS + y_up,
            rank_x[r] * XY_CUTS + y_down,
        ]

        def count(cell):
            cell = cell.astype(f32)
            return sum(jnp.where(rank == cell, 1.0, 0.0) for rank in ranks_of)

        return count

    z_lane = iota(wide, 1)

    def z_pair(values, z_lane):
        before = jnp.where(z_lane == 0, 0.0, pltpu.roll(values, 1, 1))
        after = jnp.where(z_lane == cells_z - 1, 0.0, pltpu.roll(values, cells_z - 1, 1))
        return before + after

    def correct(rhs, store):
        line = jnp.concatenate([rhs[0:1], rhs[1:2]], axis=1)
        at = iota((8, coarse), 0)
        left = jnp.zeros((8, coarse), f32)
        for n, part in enumerate(split3(line)):
            left = jnp.where(at == n, part.astype(f32), left)
        left = left.astype(bf16)
        solved = dot(left, inverse_parts[0], NT)
        solved = solved + jnp.where(at < 2, dot(left, inverse_parts[1], NT), 0.0)
        solved = solved + jnp.where(at < 1, dot(left, inverse_parts[2], NT), 0.0)
        solved = jnp.sum(solved, axis=0, keepdims=True)
        pairs = XY_CUTS * XY_CUTS
        row = iota((pairs, coarse), 0)
        column = iota((pairs, coarse), 1)
        spread = jnp.where(
            column // Z_CUTS == row, jnp.broadcast_to(solved, (pairs, coarse)), 0.0
        )
        parts = dot(jnp.concatenate(split3(spread), axis=0), map_g[...], NN)
        boxes = parts[:pairs] + parts[pairs : 2 * pairs] + parts[2 * pairs :]
        by_x = []
        for a in range(XY_CUTS):
            picked = jnp.zeros(wide, f32)
            for b in range(XY_CUTS):
                line = boxes[a * XY_CUTS + b : a * XY_CUTS + b + 1]
                picked = jnp.where(rank_y_wide == float(b), jnp.broadcast_to(line, wide), picked)
            by_x.append(picked)
        for r in range(n_ext):
            height = rows_y if r in (0, n_ext - 1) else 2 * rows_y
            picked = jnp.zeros((height, cells_z), f32)
            for a in range(XY_CUTS):
                here = rank_x_wide[r][:height] == float(a)
                picked = jnp.where(here, by_x[a][:height], picked)
            store(r, pl.ds(0, height), picked)

    def sweep(old, new, r):
        here = old[r]
        around = old[r - 1] + old[r + 1]
        around = around + pltpu.roll(here, 1, 0) + pltpu.roll(here, 2 * rows_y - 1, 0)
        around = around + z_pair(here, z_lane)
        new[r] = here * THIRD + weighted_q[r] + weight[r] * around

    def smooth(last):
        fields = (field_a, field_b)
        for s in range(SWEEPS):
            for r in range(1 + s, n_ext - 1 - s):
                if s == SWEEPS - 1:
                    last(r, fields[s % 2])
                elif r in (1 + s, n_ext - 2 - s):
                    value = last_value(r, fields[s % 2])
                    fields[1 - s % 2][r, pl.ds(0, rows_y), :] = value
                else:
                    sweep(fields[s % 2], fields[1 - s % 2], r)

    own_lane = iota((rows_y, cells_z), 1)

    def last_value(r, old):
        here = old[r]
        around = old[r - 1, pl.ds(0, rows_y), :] + old[r + 1, pl.ds(0, rows_y), :]
        beside_y = pltpu.roll(here, 1, 0) + pltpu.roll(here, 2 * rows_y - 1, 0)
        here = here[:rows_y]
        around = around + beside_y[:rows_y] + z_pair(here, own_lane)
        own = pl.ds(0, rows_y)
        return here * THIRD + weighted_q[r, own, :] + weight[r, own, :] * around

    def store_first(r, rows, picked):
        field_a[r, rows, :] = picked

    rhs = end_sum(0)
    correct(rhs, store_first)

    def last_first(r, old):
        ext_p[r, pl.ds(0, rows_y), :] = last_value(r, old)

    smooth(last_first)

    terms, stack = [], []
    for x in range(rows_x):
        p = ext_p[HALO + x, pl.ds(0, rows_y), :]
        stack.append(source_ref[x] - (6.0 + diagonal_ref[x]) * p + z_pair(p, own_lane))
    for x in range(rows_x):
        stack.append(ext_p[HALO + x, pl.ds(0, rows_y), :])
    values = along_z(jnp.concatenate(stack, axis=0))
    for x in range(2 * rows_x):
        count = same(box[x]) if x < rows_x else beside(x - rows_x)
        terms.append((values[x * rows_y : (x + 1) * rows_y], count))
    halves = to_boxes(terms)
    start_sum(1, halves)
    pressure_copies = len(halo_copies)
    own_p = ext_p.at[pl.ds(HALO, rows_x), pl.ds(0, rows_y), :]
    send_sides(own_p, ext_p, HALO, 16, True)

    middle_sum(1)
    send_sides(own_p, ext_p, HALO, 16, False)
    for copy in halo_copies[pressure_copies:]:
        copy.wait_recv()

    def store_second(r, rows, picked):
        height = picked.shape[0]
        here = (rank_x_wide[r][:height] >= 0.0) & (rank_y_wide[:height] >= 0.0)
        field_a[r, rows, :] = picked + jnp.where(here, ext_p[r, rows, :], 0.0)

    rhs = end_sum(1)
    correct(rhs, store_second)

    def last_second(r, old):
        final[pl.ds((r - HALO) * rows_y, rows_y), :] = last_value(r, old)

    smooth(last_second)

    n_far = n_grp // 2
    own_cells = pl.ds(pl.multiple_of(grp * per_k, per_k), per_k)
    pair_at = lax.div(grp, n_far) * n_far
    far_at = n_far - pair_at
    core_at = grp - pair_at
    others = [(0, far_at + lax.rem(core_at + i, n_far)) for i in range(n_far)]
    others += [(1, pair_at + lax.rem(core_at + i, n_far)) for i in range(1, n_far)]
    for n, (near_by, other) in enumerate(others):
        lanes = pl.ds(pl.multiple_of(other * LANES, LANES), LANES)
        copy = remote(final.at[:, lanes], snap.at[own_cells],
                      snap_send.at[n], snap_recv.at[near_by], (other, gx, gy))
        ends.append(copy.wait_send)
    own_lanes = pl.ds(pl.multiple_of(grp * LANES, LANES), LANES)
    snap[own_cells, :] = final[:, own_lanes]

    def products(base):
        def step(at, carry):
            rows = [
                jnp.broadcast_to(snap[pl.ds((base + t) * per_k + at, 1), :], (8, LANES))
                for t in range(n_far)
            ]
            out = []
            for kt in range(k_all // 8):
                taken = packed[kt, at]
                for t in range(n_far):
                    out.append(carry[kt * n_far + t] + taken * rows[t])
            return tuple(out)

        zeros = tuple(jnp.zeros((8, LANES), f32) for _ in range(k_all // 8 * n_far))
        sums = lax.fori_loop(0, per_k, step, zeros, unroll=4)
        for kt in range(k_all // 8):
            for t in range(n_far):
                to = pl.multiple_of((base + t) * k_all, 8) + kt * 8
                reduced[pl.ds(to, 8), :] = sums[kt * n_far + t]

    wait_bytes(snap.at[pl.ds(0, (n_far - 1) * per_k)], snap_recv.at[1])
    products(pair_at)
    wait_bytes(snap.at[pl.ds(0, n_far * per_k)], snap_recv.at[0])
    products(far_at)
    ones = jnp.ones((16, LANES), bf16)
    sums = sum(dot(ones, part, NT)[0:1] for part in split3(reduced[...]))
    n_out = n_grp * k_all
    for i in range(n_out // LANES):
        out_send[0, pl.ds(i, 1), :] = sums[:, i * LANES : (i + 1) * LANES]
    for i in range(n_out // LANES, 4):
        out_send[0, pl.ds(i, 1), :] = jnp.zeros((1, LANES), f32)
    all_at = grp * n_plane + plane_at
    summing = core_at == n_far - 1
    partner = (grp + 1 - 2 * core_at, gx, gy)
    pair_index = lax.div(grp, n_far)
    chips = []
    for i in range(n_grp // n_far):
        for j in range(n_low):
            for k in range(n_gy):
                who = (
                    lax.rem(pair_index + i, n_grp // n_far) * n_far + n_far - 1,
                    lax.rem(gx + j * n_z, n_gx),
                    lax.rem(gy + k, n_gy),
                )
                chips.append((2 * i + j + min(k, n_gy - k), who))
    chips = [who for away, who in sorted(chips, key=lambda chip: -chip[0]) if away]
    pout[all_at] = out_send[0]
    for who in chips:
        remote(out_send.at[0], pout.at[all_at], sum_send_sem.at[2, 0], sum_recv_sem.at[2, 0], who)
    ends.append(lambda: wait_bytes(pout.at[pl.ds(0, len(chips))], sum_send_sem.at[2, 0]))

    @pl.when(jnp.logical_not(summing))
    def _():
        remote(out_send.at[0], pout.at[all_at], pair_send.at[0], sum_recv_sem.at[2, 0], partner)

    n_all = n_grp * n_plane

    take_loads(2)

    def add_range(k, carry):
        total = range_in[k]
        for t in range(n_grp):
            total = total + omega_ref[t, k] * snap[pl.ds(t * per_k, per_k), :]
        range_done[k] = total
        return carry

    lax.fori_loop(0, range_in.shape[0], add_range, 0)

    @pl.when(summing)
    def _():
        wait_bytes(pout.at[pl.ds(0, n_all - 1)], sum_recv_sem.at[2, 0])
        total = pout[0]
        for i in range(1, n_all):
            total = total + pout[i]
        out_send[1] = total
        zout[z_at] = out_send[1]
        for _, who_x, who_y in far_first:
            for who in ((partner[0], who_x, who_y), (grp, who_x, who_y)):
                remote(out_send.at[1], zout.at[z_at],
                       sum_send_sem.at[2, 1], sum_recv_sem.at[2, 1], who)
        remote(out_send.at[1], zout.at[z_at], sum_send_sem.at[2, 1], sum_recv_sem.at[2, 1], partner)

    n_core = xi_ref.shape[1]
    by_t = iota((n_out, n_core), 0) // k_all
    columns = jnp.zeros((n_out, n_core), f32)
    for t in range(n_grp):
        line = jnp.broadcast_to(xi_ref[pl.ds(t, 1), :], (n_out, n_core))
        columns = jnp.where(by_t == t, line, columns)
    row_pick = iota((n_out, n_core), 0) % k_all == iota((n_out, n_core), 1)
    right = [part.astype(f32) for part in split3(columns)]
    right.append(jnp.where(row_pick, 1.0, 0.0))
    right = jnp.concatenate(right, axis=1).astype(bf16)
    core_pick = iota((k_phi, n_out), 1) % k_all == iota((k_phi, n_out), 0) + k_psi
    t_pick = iota((16, n_out), 1) // k_all == iota((16, n_out), 0)
    for end in ends:
        end()

    @pl.when(summing)
    def _():
        wait_bytes(zout.at[pl.ds(0, n_z - 1)], sum_recv_sem.at[2, 1])

    @pl.when(jnp.logical_not(summing))
    def _():
        wait_bytes(zout, sum_recv_sem.at[2, 1])

    total = zout[0]
    for i in range(1, n_z):
        total = total + zout[i]
    line = jnp.concatenate([total[i : i + 1] for i in range(n_out // LANES)], axis=1)
    left = []
    for part in split3(line):
        part = part.astype(f32)
        left.append(jnp.where(core_pick, jnp.broadcast_to(part, (k_phi, n_out)), 0.0))
        left.append(jnp.where(t_pick, jnp.broadcast_to(part, (16, n_out)), 0.0))
    parts = dot(jnp.concatenate(left, axis=0).astype(bf16), right, NN)
    n = k_phi + 16
    result = parts[:n] + parts[n : 2 * n] + parts[2 * n :]
    images = result[:k_phi]
    core_sum = images[:, :n_core] + images[:, n_core : 2 * n_core] + images[:, 2 * n_core : 3 * n_core]
    core_out[...] = core_ref[...] + core_sum
    corange_out[...] = result[k_phi : k_phi + n_grp, 3 * n_core : 3 * n_core + k_psi]

    @pl.when(summing)
    def _():
        wait_bytes(pout.at[pl.ds(0, 2 * n_z - 1)], sum_send_sem.at[2, 1])

    @pl.when(jnp.logical_not(summing))
    def _():
        wait_bytes(pout.at[0], pair_send.at[0])


def finish(range_in, corange_in, core_in, range_out, corange_out, core_out, sems):
    pairs = ((range_in, range_out), (corange_in, corange_out), (core_in, core_out))
    stores = [pltpu.make_async_copy(src, dst, sems.at[n]) for n, (src, dst) in enumerate(pairs)]
    for store in stores:
        store.start()
    for store in stores:
        store.wait()


def solution(mesh):
    n_grp, n_gx, n_gy = (mesh.shape[name] for name in ("grp", "gx", "gy"))
    n_z = min(16, n_gx // 2)
    n_low = n_gx // n_z

    def body(
        sources,
        diagonal,
        coarse_ids,
        coarse_inverse,
        omega_rows,
        psi,
        phi,
        xi_cols,
        range_sketch,
        core_sketch,
    ):
        _, rows_x, rows_y, cells_z = sources.shape
        total_cells = rows_x * n_gx * rows_y * n_gy * cells_z
        k_psi, k_phi = psi.shape[0], phi.shape[0]
        k_all = k_psi + k_phi
        k_range = range_sketch.shape[0]
        n_ext = rows_x + 2 * HALO
        per_k = rows_x * rows_y
        coarse = coarse_inverse.shape[0]
        vmem = pl.BlockSpec(memory_space=pltpu.VMEM)
        hbm = pl.BlockSpec(memory_space=pl.ANY)
        ext = pltpu.VMEM((n_ext, 2 * rows_y, cells_z), f32)
        call = pl.pallas_call(
            functools.partial(kernel, (n_grp, n_gx, n_gy, n_z, total_cells)),
            out_shape=(
                pltpu.VMEM((k_range, per_k, LANES), f32),
                pltpu.VMEM((n_grp, k_psi), f32),
                pltpu.VMEM(core_sketch.shape, f32),
            ),
            in_specs=[hbm] * 10,
            out_specs=(vmem, vmem, vmem),
            scratch_shapes=[
                pltpu.VMEM((rows_x, rows_y, cells_z), f32),
                pltpu.VMEM((rows_x, rows_y, cells_z), f32),
                pltpu.VMEM((rows_x, rows_y, cells_z), jnp.int32),
                pltpu.VMEM(coarse_inverse.shape, f32),
                pltpu.SMEM(omega_rows.shape, f32),
                pltpu.VMEM((n_grp, xi_cols.shape[0]), f32),
                pltpu.VMEM(core_sketch.shape, f32),
                pltpu.VMEM((k_all * per_k, LANES), f32),
                pltpu.VMEM((k_range, per_k, LANES), f32),
                ext,
                ext,
                ext,
                ext,
                ext,
                ext,
                ext,
                pltpu.VMEM((per_k, cells_z), f32),
                pltpu.VMEM((n_grp * per_k, LANES), f32),
                pltpu.VMEM((k_all // 8, per_k, 8, LANES), f32),
                pltpu.VMEM((n_grp * k_all, LANES), f32),
                pltpu.VMEM((2, rows_y, LANES), f32),
                pltpu.VMEM((4, 2, rows_y, LANES), f32),
                pltpu.VMEM((LANES, cells_z), bf16),
                pltpu.VMEM((coarse, cells_z), bf16),
                pltpu.VMEM((2, 2, 2, LANES), f32),
                pltpu.VMEM((2, n_z, 2, LANES), f32),
                pltpu.VMEM((2, n_low * n_gy, 2, LANES), f32),
                pltpu.VMEM((2, 4, LANES), f32),
                pltpu.VMEM((n_z, 4, LANES), f32),
                pltpu.VMEM((n_grp * n_low * n_gy, 4, LANES), f32),
                pltpu.SemaphoreType.DMA((10,)),
                pltpu.SemaphoreType.DMA((28,)),
                pltpu.SemaphoreType.DMA((28,)),
                pltpu.SemaphoreType.DMA((3, 2)),
                pltpu.SemaphoreType.DMA((3, 2)),
                pltpu.SemaphoreType.DMA((n_grp - 1,)),
                pltpu.SemaphoreType.DMA((2,)),
                pltpu.SemaphoreType.REGULAR((2,)),
                pltpu.VMEM((3, coarse, coarse), bf16),
                pltpu.SemaphoreType.DMA((1,)),
            ],
            compiler_params=pltpu.CompilerParams(
                collective_id=0, has_side_effects=True
            ),
            name="two_level_sketch",
        )
        range_new, corange_cols, core_new = call(
            sources[0],
            diagonal,
            coarse_ids,
            coarse_inverse,
            omega_rows,
            psi.reshape(k_psi * per_k, LANES),
            phi.reshape(k_phi * per_k, LANES),
            xi_cols.T,
            range_sketch.reshape(k_range, per_k, LANES),
            core_sketch,
        )
        range_new, corange_cols, core_new = pl.pallas_call(
            finish,
            out_shape=(
                jax.ShapeDtypeStruct((k_range, per_k, LANES), f32),
                jax.ShapeDtypeStruct((n_grp, k_psi), f32),
                jax.ShapeDtypeStruct(core_sketch.shape, f32),
            ),
            in_specs=[vmem] * 3,
            out_specs=(hbm, hbm, hbm),
            scratch_shapes=[pltpu.SemaphoreType.DMA((3,))],
            compiler_params=pltpu.CompilerParams(vmem_limit_bytes=1 << 21),
            name="finish",
        )(range_new, corange_cols, core_new)
        return range_new.reshape(range_sketch.shape), corange_cols.T, core_new

    return jax.shard_map(
        body,
        mesh=mesh,
        in_specs=(
            P("grp", "gx", "gy", None),
            P("gx", "gy", None),
            P("gx", "gy", None),
            P(),
            P(),
            P(None, "gx", "gy", "grp"),
            P(None, "gx", "gy", "grp"),
            P(),
            P(None, "gx", "gy", "grp"),
            P(),
        ),
        out_specs=(P(None, "gx", "gy", "grp"), P(), P()),
        check_vma=False,
    )
```
